32 devices in a mesh: fsdp: 16 (over z, y, x), tp: 2 (over core).
Axes of the slice: x: 2, y: 2, z: 4, core: 2. Of those that a mesh axis runs over, the one named last changes fastest.
Arguments:
- hidden_in: bfloat16 [16384, 1152], P(('fsdp', 'tp')), may hold values from -6 to 6
- out_grad: bfloat16 [16384, 1152], P(('fsdp', 'tp')), may hold values from -6 to 6
- segments: int32 [16384], P('fsdp'), may hold values from 0 to 17, as said below
- positions: int32 [16384], P('fsdp'), may hold values from 0 to 799, as said below
- set_ids: int32 [16], replicated, may hold values from 0 to 7, as said below
- query_w: bfloat16 [2, 1152, 1024], P(None, 'fsdp', 'tp'), may hold values from -0.1875 to 0.1875
- key_w: bfloat16 [2, 1152, 256], P(None, 'fsdp'), may hold values from -0.1875 to 0.1875
- value_w: bfloat16 [2, 1152, 256], P(None, 'fsdp'), may hold values from -0.1875 to 0.1875
- out_w: bfloat16 [2, 1024, 1152], P(None, 'tp', 'fsdp'), may hold values from -0.1875 to 0.1875
- gate_w: bfloat16 [2, 1152, 6912], P(None, 'fsdp', 'tp'), may hold values from -0.1875 to 0.1875
- up_w: bfloat16 [2, 1152, 6912], P(None, 'fsdp', 'tp'), may hold values from -0.1875 to 0.1875
- down_w: bfloat16 [2, 6912, 1152], P(None, 'tp', 'fsdp'), may hold values from -0.078125 to 0.078125
- norm_gains: bfloat16 [2, 4, 1152], replicated, may hold values from -0.3984375 to 0.3984375
- head_gains: bfloat16 [2, 2, 256], replicated, may hold values from -0.3984375 to 0.3984375
- adapters: float32 [8, 1003520], P(None, ('fsdp', 'tp')), may hold values from -0.18 to 0.18
- first_moment: float32 [8, 1003520], P(None, ('fsdp', 'tp')), may hold values from -1122 to 1122
- second_moment: float32 [8, 1003520], P(None, ('fsdp', 'tp')), may hold values from 4371 to 69938
Outputs:
- second_layer_output: bfloat16 [16384, 1152], P(('fsdp', 'tp'))
- input_grad: float32 [16384, 1152], P(('fsdp', 'tp'))
- adapter_grads: float32 [8, 1003520], P(None, ('fsdp', 'tp'))
- new_adapters: float32 [8, 1003520], P(None, ('fsdp', 'tp'))
- new_first: float32 [8, 1003520], P(None, ('fsdp', 'tp'))
- new_second: float32 [8, 1003520], P(None, ('fsdp', 'tp'))
- adapter_copy: bfloat16 [8, 1003520], P(None, ('fsdp', 'tp'))
The draws below stay inside these ranges and needn't reach their ends.
Inputs may be any that keep to these rules, and one draw needn't show every extreme that they name: `segments`: within each sequence of 1024 tokens the document number starts at 0 and rises by one at each new document; every document that ends inside its sequence has 60 to 800 tokens, the last one of a sequence 1 to 800; some document has exactly 800 tokens, and some sequence holds the most documents that these bounds allow. `positions`: each token's offset from the first token of its document. `set_ids`: every one of the 8 sets is used by at least one sequence.
All inputs are finite; a program needn't handle non-finite values.
Results may differ from the reference program's by a relative error of at most 0.028.
Values may be sent and summed in bfloat16 or wider, within the bound.
A program may use at most 448 MiB of HBM per device.

```python
import math
import jax
import jax.numpy as jnp
from jax import lax

D = 1152
HEADS = 4
HD = 256
FF = 6912
WINDOW = 512
RANK = 16
SETS = 8
LAYERS = 2
DOC_MIN = 60
DOC_MAX = 800
LENGTH = 1024
TOKENS = 16384
PARAMS = 1003520
MOMENT_SPREAD = 187


def doc_layout(key):
    seq_count = TOKENS // LENGTH
    doc_slots = LENGTH // DOC_MIN + 2
    length_key = jax.random.fold_in(key, 11)
    pick_key = jax.random.fold_in(key, 12)
    spans = jax.random.randint(length_key, (seq_count, doc_slots), DOC_MIN, DOC_MAX + 1).astype(jnp.int32)
    chosen = jax.random.randint(pick_key, (), 0, seq_count)
    packed_row = (chosen + 1) % seq_count
    first_col = jnp.arange(doc_slots) == 0
    chosen_row = jnp.arange(seq_count) == chosen
    dense_row = jnp.arange(seq_count) == packed_row
    spans = jnp.where(dense_row[:, None], DOC_MIN, spans).astype(jnp.int32)
    spans = jnp.where(chosen_row[:, None] & first_col[None, :], DOC_MAX, spans).astype(jnp.int32)
    ends = jnp.cumsum(spans, axis=1).astype(jnp.int32)
    starts = ends - spans
    cells = jnp.arange(LENGTH, dtype=jnp.int32)
    doc_index = jnp.sum((ends[:, None, :] <= cells[None, :, None]).astype(jnp.int32), axis=2).astype(jnp.int32)
    doc_start = jnp.take_along_axis(starts, doc_index, axis=1)
    offsets = (cells[None, :] - doc_start).astype(jnp.int32)
    return (doc_index.reshape(-1), offsets.reshape(-1))


def draw_segments(key, part):
    return doc_layout(key)[0]


def draw_positions(key, part):
    return doc_layout(key)[1]


def draw_set_ids(key, part):
    seq_count = TOKENS // LENGTH
    random_sets = jax.random.randint(jax.random.fold_in(key, 21), (seq_count,), 0, SETS).astype(jnp.int32)
    slot_index = jnp.arange(seq_count, dtype=jnp.int32)
    covered = jnp.where(slot_index < SETS, slot_index % SETS, random_sets).astype(jnp.int32)
    shuffle = jax.random.permutation(jax.random.fold_in(key, 22), seq_count)
    return covered[shuffle].astype(jnp.int32)


def block_levels(own_key, extent, split, least, high):
    gain, own = 1.0, jax.random.fold_in(own_key, 6)
    for position, parts in split:
        steps = jnp.exp(jax.random.uniform(jax.random.fold_in(own, position), (parts,), jnp.float32, least / len(split), high / len(split)))
        gain = gain * jnp.repeat(steps, extent[position] // parts).reshape([-1 if axis == position else 1 for axis in range(len(extent))])
    return gain


def normal_values(stream_key, shape, deviation, reach, cuts=(), kind=jnp.bfloat16):
    values = deviation * jax.random.normal(stream_key, shape, jnp.float32)
    if cuts:
        values = values * block_levels(stream_key, shape, cuts, -0.22, 0.18)
    return jnp.clip(values, -reach, reach).astype(kind)


def setup_inputs(seed: int = 0) -> dict:
    key_list = jax.random.split(jax.random.key(seed), 18)
    hidden_in = normal_values(key_list[0], (TOKENS, D), 1.0, 6.0, ((0, 32),))
    out_grad = normal_values(key_list[1], (TOKENS, D), 1.0, 6.0, ((0, 32),))
    segments = draw_segments(jax.random.fold_in(key_list[17], 71), 0)
    positions = draw_positions(jax.random.fold_in(key_list[17], 71), 0)
    set_ids = draw_set_ids(jax.random.fold_in(key_list[17], 71), 0)
    query_w = normal_values(key_list[5], (LAYERS, D, HEADS * HD), D ** -0.5, 0.1875, ((1, 16), (2, 2)))
    key_w = normal_values(key_list[6], (LAYERS, D, HD), D ** -0.5, 0.1875, ((1, 16),))
    value_w = normal_values(key_list[7], (LAYERS, D, HD), D ** -0.5, 0.1875, ((1, 16),))
    out_w = normal_values(key_list[8], (LAYERS, HEADS * HD, D), (HEADS * HD) ** -0.5, 0.1875, ((1, 2), (2, 16)))
    gate_w = normal_values(key_list[9], (LAYERS, D, FF), D ** -0.5, 0.1875, ((1, 16), (2, 2)))
    up_w = normal_values(key_list[10], (LAYERS, D, FF), D ** -0.5, 0.1875, ((1, 16), (2, 2)))
    down_w = normal_values(key_list[11], (LAYERS, FF, D), FF ** -0.5, 0.078125, ((1, 2), (2, 16)))
    norm_gains = jnp.clip(jax.random.uniform(key_list[12], (LAYERS, 4, D), jnp.float32, -0.3984375, 0.3984375), -0.3984375, 0.3984375).astype(jnp.bfloat16)
    head_gains = jnp.clip(jax.random.uniform(key_list[13], (LAYERS, 2, HD), jnp.float32, -0.3984375, 0.3984375), -0.3984375, 0.3984375).astype(jnp.bfloat16)
    adapters = normal_values(key_list[14], (SETS, PARAMS), 0.03, 0.18, ((1, 32),), jnp.float32)
    first_moment = normal_values(key_list[15], (SETS, PARAMS), MOMENT_SPREAD, 1122.0, ((1, 32),), jnp.float32)
    second_moment = jnp.clip(jnp.exp(math.log(69938.0) - 2.7726173 * jax.random.uniform(key_list[16], (SETS, PARAMS), jnp.float32) ** block_levels(key_list[16], (SETS, PARAMS), ((1, 32),), -0.2, 0.2)), 4371.0, 69938.0)
    return {"hidden_in": hidden_in, "out_grad": out_grad, "segments": segments, "positions": positions, "set_ids": set_ids, "query_w": query_w, "key_w": key_w, "value_w": value_w, "out_w": out_w, "gate_w": gate_w, "up_w": up_w, "down_w": down_w, "norm_gains": norm_gains, "head_gains": head_gains, "adapters": adapters, "first_moment": first_moment, "second_moment": second_moment}


NORM_EPS = 1e-06
ADAPTER_SCALING = 4.0
ROPE_BASE = 10000.0
LEARN_RATE = 0.01
BETA_ONE = 0.5
BETA_TWO = 0.6
ADAM_STEPS = 4.0
ADAM_EPS = 1e-08
DECAY_RATE = 0.1
NEG_FILL = -1e+30
MAXIMAL_PRECISION = lax.Precision.HIGHEST

@jax.custom_vjp
def low(v):
    return lax.optimization_barrier(v.astype(jnp.bfloat16)).astype(jnp.float32)

@jax.custom_vjp
def low_back(v):
    return v

def low_keep(v):
    return (low(v), None)

def low_pass(kept, grad):
    return (grad,)

def back_keep(v):
    return (v, None)

def back_low(kept, grad):
    return (low(grad),)
low.defvjp(low_keep, low_pass)
low_back.defvjp(back_keep, back_low)

def adapter_shapes():
    heads_width = HEADS * HD
    return [(D, RANK), (RANK, heads_width), (D, RANK), (RANK, HD), (D, RANK), (RANK, HD), (heads_width, RANK), (RANK, D), (D, RANK), (RANK, FF), (D, RANK), (RANK, FF), (FF, RANK), (RANK, D)]

def unpack_layer(flat_values, layer_idx):
    shapes = adapter_shapes()
    stride = sum((height * breadth for height, breadth in shapes))
    offset = layer_idx * stride
    pieces = []
    for height, breadth in shapes:
        pieces.append(flat_values[offset:offset + height * breadth].reshape(height, breadth))
        offset = offset + height * breadth
    return pieces

def norm_rows(values, gain_vec):
    return values * lax.rsqrt(lax.optimization_barrier(jnp.mean(values * values, axis=-1, keepdims=True)) + NORM_EPS) * (1.0 + gain_vec)

def rotate(values, places):
    half_width = values.shape[-1] // 2
    frequency = jnp.exp(jnp.arange(half_width, dtype=jnp.float32) * (-2.0 * math.log(ROPE_BASE) / values.shape[-1]))
    angles = places.astype(jnp.float32)[:, None] * frequency[None, :]
    cosine = jnp.cos(angles)[:, None, :]
    sine_part = jnp.sin(angles)[:, None, :]
    front_half = values[..., :half_width]
    back_half = values[..., half_width:]
    return jnp.concatenate([front_half * cosine - back_half * sine_part, back_half * cosine + front_half * sine_part], axis=-1)

def prep_heads(raw_rows, gain_vec, places):
    shaped = raw_rows.reshape(raw_rows.shape[0], raw_rows.shape[1] // gain_vec.shape[0], gain_vec.shape[0])
    return rotate(norm_rows(shaped, gain_vec), places)

def adapter_out(inputs, entry_map, leaving_projection):
    inner_rows = jnp.dot(inputs, entry_map, precision=MAXIMAL_PRECISION)
    return ADAPTER_SCALING * jnp.dot(inner_rows, leaving_projection, precision=MAXIMAL_PRECISION)

def project(inputs, weight_mat, entry_map, leaving_projection):
    return jnp.dot(inputs, weight_mat, precision=MAXIMAL_PRECISION) + adapter_out(inputs, entry_map, leaving_projection)

def attention(queries, key_rows, value_matrix_rows, segment_ids):
    cells = jnp.arange(queries.shape[0])
    offsets = cells[:, None] - cells[None, :]
    allowed = (offsets >= 0) & (offsets < WINDOW) & (segment_ids[:, None] == segment_ids[None, :])
    raw_scores = low_back(jnp.einsum('qhd,kd->hqk', queries, key_rows, precision=MAXIMAL_PRECISION) * HD ** (-0.5))
    masked = jnp.where(allowed[None], raw_scores, NEG_FILL)
    row_max = lax.optimization_barrier(jnp.max(masked, axis=-1, keepdims=True))
    expon = jnp.exp(masked - row_max)
    weights_low = low(expon / lax.optimization_barrier(jnp.sum(expon, axis=-1, keepdims=True)))
    mixed = jnp.einsum('hqk,kd->qhd', weights_low, value_matrix_rows, precision=MAXIMAL_PRECISION)
    return low_back(low(mixed.reshape(queries.shape[0], -1)))

def layer_forward(residual, own_set, layer_idx, weight_list, gains_all, heads_all, places, segment_ids):
    query_weight, key_weight, value_weight, out_weight, gate_weight, up_weight, down_weight = [w_all[layer_idx] for w_all in weight_list]
    layer_gains = gains_all[layer_idx]
    head_gain = heads_all[layer_idx]
    pieces = unpack_layer(own_set, layer_idx)
    normed = low(norm_rows(residual, layer_gains[0]))
    query_raw = low_back(project(normed, query_weight, pieces[0], pieces[1]))
    key_raw = project(normed, key_weight, pieces[2], pieces[3])
    value_raw = project(normed, value_weight, pieces[4], pieces[5])
    queries = low(prep_heads(query_raw, head_gain[0], places))
    key_rows = low(prep_heads(key_raw, head_gain[1], places)[:, 0, :])
    value_matrix_rows = low(value_raw)
    attn_out = attention(queries, key_rows, value_matrix_rows, segment_ids)
    attn_branch = low_back(project(attn_out, out_weight, pieces[6], pieces[7]))
    inner_rows = residual + norm_rows(attn_branch, layer_gains[1])
    normed_two = low(norm_rows(inner_rows, layer_gains[2]))
    gate_pre = low_back(project(normed_two, gate_weight, pieces[8], pieces[9]))
    up_pre = low_back(project(normed_two, up_weight, pieces[10], pieces[11]))
    hidden = low(jax.nn.gelu(gate_pre, approximate=True) * up_pre)
    ffn_branch = low_back(project(hidden, down_weight, pieces[12], pieces[13]))
    return inner_rows + norm_rows(ffn_branch, layer_gains[3])

def reference(hidden_in, out_grad, segments, positions, set_ids, query_w, key_w, value_w, out_w, gate_w, up_w, down_w, norm_gains, head_gains, adapters, first_moment, second_moment):
    seq_count = TOKENS // LENGTH
    weight_list = [w_all.astype(jnp.float32) for w_all in (query_w, key_w, value_w, out_w, gate_w, up_w, down_w)]
    gains_all = norm_gains.astype(jnp.float32)
    heads_all = head_gains.astype(jnp.float32)
    segment_rows = segments.reshape(seq_count, LENGTH)
    place_rows = positions.reshape(seq_count, LENGTH)

    def forward(start_rows, master):
        copies = low(master)

        def one_sequence(items):
            rows_in, segment_ids, places, chosen = items
            own_set = lax.dynamic_index_in_dim(copies, chosen, 0, keepdims=False)
            state = rows_in
            for layer_idx in range(LAYERS):
                state = layer_forward(state, own_set, layer_idx, weight_list, gains_all, heads_all, places, segment_ids)
            return state
        outputs = lax.map(jax.checkpoint(one_sequence), (start_rows.reshape(seq_count, LENGTH, D), segment_rows, place_rows, set_ids))
        return outputs.reshape(TOKENS, D)
    result, backward = jax.vjp(forward, hidden_in.astype(jnp.float32), adapters)
    input_grad, adapter_grads = backward(out_grad.astype(jnp.float32))
    first_new = BETA_ONE * first_moment + (1.0 - BETA_ONE) * adapter_grads
    second_new = BETA_TWO * second_moment + (1.0 - BETA_TWO) * adapter_grads * adapter_grads
    first_hat = first_new / (1.0 - BETA_ONE ** ADAM_STEPS)
    second_hat = second_new / (1.0 - BETA_TWO ** ADAM_STEPS)
    new_master = adapters - LEARN_RATE * (first_hat / (jnp.sqrt(second_hat) + ADAM_EPS) + DECAY_RATE * adapters)
    return (result.astype(jnp.bfloat16), input_grad, adapter_grads, new_master, first_new, second_new, new_master.astype(jnp.bfloat16))
```

```python
import functools
import math

import jax
import jax.numpy as jnp
from jax import lax
from jax.experimental import pallas as pl
from jax.experimental.pallas import tpu as pltpu
from jax.sharding import PartitionSpec as P

D = 1152
HEADS = 4
HD = 256
FF = 6912
WINDOW = 512
RANK = 16
LAYERS = 2
LANES = 128
GROUPS = LANES // RANK

NORM_EPS = 1e-06
ADAPTER_SCALING = 4.0
ROPE_BASE = 10000.0
LEARN_RATE = 0.01
BETA_ONE = 0.5
BETA_TWO = 0.6
ADAM_STEPS = 4.0
ADAM_EPS = 1e-08
DECAY_RATE = 0.1
NEG_FILL = -1e30
F32 = jnp.float32
BF16 = jnp.bfloat16
MESH = pl.DeviceIdType.MESH

PIECES = (
    ("Eq", D), ("Xq", HEADS * HD), ("Ek", D), ("Xk", HD), ("Ev", D), ("Xv", HD),
    ("Eo", HEADS * HD), ("Xo", D), ("Eg", D), ("Xg", FF), ("Eu", D), ("Xu", FF),
    ("Ed", FF), ("Xd", D),
)


def dot(a, b, out=F32):
    return lax.dot_general(a, b, (((1,), (0,)), ((), ())), preferred_element_type=F32).astype(out)


def dot_nt(a, b, out=F32):
    return lax.dot_general(a, b, (((1,), (1,)), ((), ())), preferred_element_type=F32).astype(out)


def dot_tn(a, b, out=F32):
    return lax.dot_general(a, b, (((0,), (0,)), ((), ())), preferred_element_type=F32).astype(out)


def rms(v, gain):
    return v * lax.rsqrt(jnp.mean(v * v, axis=-1, keepdims=True) + NORM_EPS) * (1.0 + gain)


def rms_back(v, gain, dy):
    r = lax.rsqrt(jnp.mean(v * v, axis=-1, keepdims=True) + NORM_EPS)
    scaled = (1.0 + gain) * dy
    return r * scaled - v * (r * r * r) * jnp.mean(v * scaled, axis=-1, keepdims=True)


def exchange_kernel(body, has_partial, n_rows, n_gains, n_outs, has_send, n_chunks, *refs):
    refs = list(refs)
    partial = refs.pop(0) if has_partial else None
    rows = [refs.pop(0) for _ in range(n_rows)]
    gains = [refs.pop(0) for _ in range(n_gains)]
    outs = [refs.pop(0) for _ in range(n_outs)]
    gathered = refs.pop(0) if has_send else None
    if has_partial:
        arrived, send_a, recv_a = refs[:3]
        refs = refs[3:]
    if has_send:
        send_b, recv_b = refs[:2]
    me = lax.axis_index("tp")
    other = 1 - me
    barrier = pltpu.get_barrier_semaphore()
    pl.semaphore_signal(barrier, inc=1, device_id={"tp": other}, device_id_type=MESH)
    pl.semaphore_wait(barrier, 1)
    half = (partial if has_partial else gathered).shape[0] // 2
    chunk = half // n_chunks

    def span(base, c):
        return pl.ds(pl.multiple_of(base * half + c * chunk, chunk), chunk)

    sends = []
    if has_partial:
        for c in range(n_chunks):
            copy = pltpu.make_async_remote_copy(
                src_ref=partial.at[span(other, c)],
                dst_ref=arrived.at[pl.ds(c * chunk, chunk)],
                send_sem=send_a.at[c],
                recv_sem=recv_a.at[c],
                device_id={"tp": other},
                device_id_type=MESH,
            )
            copy.start()
            sends.append(copy)
    gain_values = [g[...].astype(F32) for g in gains]
    spreads = []
    for c in range(n_chunks):
        local = pl.ds(c * chunk, chunk)
        total = None
        if has_partial:
            sends[c].wait_recv()
            total = partial[span(me, c), :].astype(F32) + arrived[local, :].astype(F32)
        values, spread = body(total, [r[local, :].astype(F32) for r in rows], gain_values)
        for ref, value in zip(outs, values):
            ref[local, :] = value.astype(ref.dtype)
        if has_send:
            gathered[span(me, c), :] = spread.astype(BF16)
            spreads.append(
                pltpu.make_async_remote_copy(
                    src_ref=gathered.at[span(me, c)],
                    dst_ref=gathered.at[span(me, c)],
                    send_sem=send_b.at[c],
                    recv_sem=recv_b.at[c],
                    device_id={"tp": other},
                    device_id_type=MESH,
                )
            )
            if c > 0:
                spreads[c - 1].start()
    if has_send:
        spreads[-1].start()
    for copy in sends:
        copy.wait_send()
    for copy in spreads:
        copy.wait()


def exchange(body, collective_id, name, partial, rows, gains, out_types, has_send, n_chunks=4):
    operands = ([] if partial is None else [partial]) + list(rows) + list(gains)
    width = operands[0].shape[1]
    half = partial.shape[0] // 2 if partial is not None else rows[0].shape[0]
    outs = [jax.ShapeDtypeStruct((half, width), kind) for kind in out_types]
    if has_send:
        outs.append(jax.ShapeDtypeStruct((2 * half, width), BF16))
    scratch = []
    if partial is not None:
        scratch += [
            pltpu.VMEM((half, width), partial.dtype),
            pltpu.SemaphoreType.DMA((n_chunks,)),
            pltpu.SemaphoreType.DMA((n_chunks,)),
        ]
    if has_send:
        scratch += [pltpu.SemaphoreType.DMA((n_chunks,)), pltpu.SemaphoreType.DMA((n_chunks,))]
    vmem = pl.BlockSpec(memory_space=pltpu.VMEM)
    return pl.pallas_call(
        functools.partial(
            exchange_kernel, body, partial is not None, len(rows), len(gains), len(out_types),
            has_send, n_chunks,
        ),
        out_shape=outs,
        in_specs=[vmem] * len(operands),
        out_specs=[vmem] * len(outs),
        scratch_shapes=scratch,
        compiler_params=pltpu.CompilerParams(collective_id=collective_id, has_side_effects=True),
        name=name,
    )(*operands)


def gather_kernel(plan, nz, rows, n_arrays, *refs):
    mine, gathered = refs[:n_arrays], refs[n_arrays : 2 * n_arrays]
    send_sem, recv_sem, local_sem = refs[2 * n_arrays :]
    f = lax.axis_index("fsdp")
    x, y, z = f % 2, (f // 2) % 2, f // 4

    def index(a, b, c):
        return (a * 2 + b) * 2 + c

    peers = {
        "x": (index(z, y, 1 - x), None),
        "y": (index(z, 1 - y, x), None),
        "u": (f + 4, z < nz - 1),
        "d": (f - 4, z > 0),
    }
    ways_index = "xyud".index

    def guarded(cond, fn):
        if cond is None:
            fn()
        else:
            pl.when(cond)(fn)

    barrier = pltpu.get_barrier_semaphore()

    def greet(peer):
        pl.semaphore_signal(barrier, inc=1, device_id={"fsdp": peer}, device_id_type=MESH)

    for peer, cond in peers.values():
        guarded(cond, functools.partial(greet, peer))
    inside = jnp.logical_and(z > 0, z < nz - 1)
    pl.when(inside)(lambda: pl.semaphore_wait(barrier, 4))
    pl.when(jnp.logical_not(inside))(lambda: pl.semaphore_wait(barrier, 3))

    offsets = [(dz, fy, fx) for dz in range(1 - nz, nz) for fy in (0, 1) for fx in (0, 1)]
    offsets.sort(key=lambda o: (abs(o[0]) + o[1] + o[2], o))
    ids = {o: i for i, o in enumerate(offsets)}
    own = (0, 0, 0)

    def place(array, source, columns):
        return gathered[array].at[pl.ds(pl.multiple_of(source * rows, 8), rows), pl.ds(*columns)]

    for a in range(n_arrays):
        pltpu.make_async_copy(
            mine[a], place(a, f, (0, mine[a].shape[1])), local_sem.at[a]
        ).start()

    def source_of(o):
        return index(z + o[0], y + o[1] - 2 * y * o[1], x + o[2] - 2 * x * o[2])

    def copy(k, o, way):
        target = {
            "u": (o[0] - 1, o[1], o[2]), "d": (o[0] + 1, o[1], o[2]),
            "x": (o[0], o[1], 1), "y": (o[0], 1, o[2]),
        }[way]
        _, array, columns = plan[k]
        block = place(array, source_of(o), columns)
        return pltpu.make_async_remote_copy(
            src_ref=mine[array].at[:, pl.ds(*columns)] if o == own else block,
            dst_ref=block,
            send_sem=send_sem.at[k, ids[o], ways_index(way)],
            recv_sem=recv_sem.at[k, ids[target]],
            device_id={"fsdp": peers[way][0]},
            device_id_type=MESH,
        )

    def arrival(k, o):
        _, array, columns = plan[k]
        block = place(array, source_of(o), columns)
        return pltpu.make_async_remote_copy(
            src_ref=block, dst_ref=block, send_sem=send_sem.at[k, ids[o], 0],
            recv_sem=recv_sem.at[k, ids[o]], device_id={"fsdp": peers["x"][0]}, device_id_type=MESH,
        )

    def ways(order, o):
        used = {"z": o[0] != 0, "y": o[1] != 0, "x": o[2] != 0}
        last = max([i for i, a in enumerate(order) if used[a]], default=-1)
        out = []
        if last >= 0 and order[last] == "z" and abs(o[0]) < nz - 1:
            out.append("d" if o[0] > 0 else "u")
        for a in order[last + 1 :]:
            out += ["u", "d"] if a == "z" else [a]
        return out

    def exists(o):
        if o[0] == 0:
            return None
        return z < nz - o[0] if o[0] > 0 else z >= -o[0]

    def pass_on(k, o):
        if o != own:
            arrival(k, o).wait_recv()
        for way in ways(plan[k][0], o):
            guarded(peers[way][1], lambda way=way: copy(k, o, way).start())

    def finish(k, o):
        for way in ways(plan[k][0], o):
            guarded(peers[way][1], lambda way=way: copy(k, o, way).wait_send())

    for step in (pass_on, finish):
        for o in offsets:
            for k in range(len(plan)):
                guarded(exists(o), functools.partial(step, k, o))
    for a in range(n_arrays):
        pltpu.make_async_copy(
            mine[a], place(a, f, (0, mine[a].shape[1])), local_sem.at[a]
        ).wait()


def gather_weights(arrays, plan, count, collective_id):
    rows = arrays[0].shape[0]
    nz = count // 4
    offsets = (2 * nz - 1) * 4
    return pl.pallas_call(
        functools.partial(gather_kernel, plan, nz, rows, len(arrays)),
        out_shape=[
            jax.ShapeDtypeStruct((count * rows, a.shape[1]), a.dtype) for a in arrays
        ],
        in_specs=[pl.BlockSpec(memory_space=pltpu.VMEM)] * len(arrays),
        out_specs=[pl.BlockSpec(memory_space=pl.ANY)] * len(arrays),
        scratch_shapes=[
            pltpu.SemaphoreType.DMA((len(plan), offsets, 4)),
            pltpu.SemaphoreType.DMA((len(plan), offsets)),
            pltpu.SemaphoreType.DMA((len(arrays),)),
        ],
        compiler_params=pltpu.CompilerParams(collective_id=collective_id, has_side_effects=True),
        name="gather_weights",
    )(*arrays)


def pair_sum_kernel(count, partial, total, arrived, send_sem, recv_sem):
    me = lax.axis_index("tp")
    other = 1 - me
    barrier = pltpu.get_barrier_semaphore()
    pl.semaphore_signal(barrier, inc=1, device_id={"tp": other}, device_id_type=MESH)
    pl.semaphore_wait(barrier, 1)
    copies = []
    for i in range(count):
        copy = pltpu.make_async_remote_copy(
            src_ref=partial.at[2 * i + other], dst_ref=arrived.at[i], send_sem=send_sem.at[i],
            recv_sem=recv_sem.at[i], device_id={"tp": other}, device_id_type=MESH,
        )
        copy.start()
        copies.append(copy)
    for i in range(count):
        copies[i].wait_recv()
        total[i] = (partial[2 * i + me].astype(F32) + arrived[i].astype(F32)).astype(total.dtype)
    for copy in copies:
        copy.wait_send()


def pair_sum(partial, collective_id):
    count = partial.shape[0] // 2
    shape = (count,) + partial.shape[1:]
    vmem = pl.BlockSpec(memory_space=pltpu.VMEM)
    return pl.pallas_call(
        functools.partial(pair_sum_kernel, count),
        out_shape=jax.ShapeDtypeStruct(shape, partial.dtype),
        in_specs=[vmem],
        out_specs=vmem,
        scratch_shapes=[
            pltpu.VMEM(shape, partial.dtype),
            pltpu.SemaphoreType.DMA((count,)),
            pltpu.SemaphoreType.DMA((count,)),
        ],
        compiler_params=pltpu.CompilerParams(collective_id=collective_id, has_side_effects=True),
        name="pair_sum",
    )(partial)


def body_enter(total, rows, gains):
    return [], rms(rows[0], gains[0])


def body_middle(total, rows, gains):
    middle = rows[0] + rms(total, gains[0])
    return [total, middle], rms(middle, gains[1])


def body_next(total, rows, gains):
    leaving = rows[0] + rms(total, gains[0])
    return [total, leaving], rms(leaving, gains[1])


def body_turn(total, rows, gains):
    leaving = rows[0] + rms(total, gains[0])
    return [leaving], rms_back(total, gains[0], rows[1])


def body_back_middle(total, rows, gains):
    grad_middle = rows[0] + rms_back(rows[1], gains[0], total)
    return [grad_middle], rms_back(rows[2], gains[1], grad_middle)


def body_back_next(total, rows, gains):
    grad_x = rows[0] + rms_back(rows[1], gains[0], total)
    return [grad_x], rms_back(rows[2], gains[1], grad_x)


def body_back_last(total, rows, gains):
    return [rows[0] + rms_back(rows[1], gains[0], total)], None


def lane_group_mask(count):
    row = lax.broadcasted_iota(jnp.int32, (count, LANES), 0)
    lane = lax.broadcasted_iota(jnp.int32, (count, LANES), 1)
    return (lane // RANK) == (row % GROUPS)


def expand_entry(flat_rows):
    count = flat_rows.shape[0] * GROUPS
    spread = jnp.broadcast_to(flat_rows[:, None, :], (flat_rows.shape[0], GROUPS, LANES))
    return jnp.where(lane_group_mask(count), spread.reshape(count, LANES), 0).astype(BF16)


def slot_pick(slot):
    row = lax.broadcasted_iota(jnp.int32, (LANES, LANES), 0)
    lane = lax.broadcasted_iota(jnp.int32, (LANES, LANES), 1)
    return (lane == slot * RANK + row % RANK).astype(BF16)


def slot_spread(slot):
    row = lax.broadcasted_iota(jnp.int32, (LANES, LANES), 0)
    lane = lax.broadcasted_iota(jnp.int32, (LANES, LANES), 1)
    return (row == slot * RANK + lane % RANK).astype(BF16)


def in_slot(rows, slot):
    return jnp.pad(rows, ((slot * RANK, LANES - (slot + 1) * RANK), (0, 0)))


def rope_tables(positions):
    half = HD // 2
    frequency = jnp.exp(jnp.arange(half, dtype=F32) * (-2.0 * math.log(ROPE_BASE) / HD))
    angles = positions.astype(F32)[:, None] * frequency[None, :]
    return jnp.cos(angles), jnp.sin(angles)


def head_forward(raw, gain, cosine, sine):
    n = rms(raw, gain)
    half = HD // 2
    a, b = n[:, :half], n[:, half:]
    return jnp.concatenate([a * cosine - b * sine, b * cosine + a * sine], axis=1)


def head_backward(raw, gain, cosine, sine, grad):
    half = HD // 2
    a, b = grad[:, :half], grad[:, half:]
    turned = jnp.concatenate([a * cosine + b * sine, b * cosine - a * sine], axis=1)
    return rms_back(raw, gain, turned)


ROW_BLOCK = 256
VMEM_LIMIT = 67000000
KEY_SPAN = WINDOW + ROW_BLOCK


def rows_at(i, count=ROW_BLOCK):
    return pl.ds(pl.multiple_of(i * count, count), count)


def key_start(i):
    return pl.multiple_of(jnp.maximum(i * ROW_BLOCK - WINDOW, 0), ROW_BLOCK)


def allowed_keys(i, first, segment_column, segment_row):
    rows = i * ROW_BLOCK + lax.broadcasted_iota(jnp.int32, (ROW_BLOCK, KEY_SPAN), 0)
    keys = first + lax.broadcasted_iota(jnp.int32, (ROW_BLOCK, KEY_SPAN), 1)
    gap = rows - keys
    same = segment_column[rows_at(i), :] == segment_row[:, pl.ds(first, KEY_SPAN)]
    return (gap >= 0) & (gap < WINDOW) & same


def weight_copies(sources, target, sems, columns=None):
    out, at = [], 0
    for i, source in enumerate(sources):
        count = source.shape[0]
        part = source if columns is None else source.at[:, columns]
        out.append(pltpu.make_async_copy(part, target.at[pl.ds(at, count)], sems.at[i]))
        at += count
    return out


def with_slots(weight):
    return pltpu.VMEM((weight.shape[0] + LANES, weight.shape[1]), BF16)


def attention_forward_kernel(
    local_heads, scale, normed, enter, leave, gains, cosine, sine, segment_column, segment_row,
    w_qkv, w_o, s_qkv, s_o, raw, qkv, attn, mid_qkv, mid_o, stats, share, w_qkv_here, w_o_here, sems,
):
    copies = [
        weight_copies((w_qkv, s_qkv), w_qkv_here, sems.at[0]),
        weight_copies((w_o, s_o), w_o_here, sems.at[1]),
    ]
    for c in copies[0] + copies[1]:
        c.start()
    blocks = normed.shape[0] // ROW_BLOCK
    key_col = local_heads * HD
    value_col = key_col + HD
    for c in copies[0]:
        c.wait()

    @pl.loop(0, blocks)
    def _(i):
        rows = rows_at(i)
        z = normed[rows, :]
        mid = dot(z, enter[...], BF16)
        mid_qkv[rows, :] = mid
        full = dot(jnp.concatenate([z, mid], axis=1), w_qkv_here[...])
        c, s = cosine[rows, :], sine[rows, :]
        for h in range(local_heads + 1):
            columns = slice(h * HD, (h + 1) * HD)
            gain = gains[0:1, :] if h < local_heads else gains[1:2, :]
            qkv[rows, columns] = head_forward(full[:, columns], gain, c, s).astype(BF16)
        raw[rows, :] = full[:, :value_col]
        qkv[rows, value_col:] = full[:, value_col:].astype(BF16)

    for c in copies[1]:
        c.wait()

    @pl.loop(0, blocks)
    def _(i):
        rows = rows_at(i)
        first = key_start(i)
        keys = qkv[pl.ds(first, KEY_SPAN), key_col:value_col]
        values = qkv[pl.ds(first, KEY_SPAN), value_col:]
        mask = allowed_keys(i, first, segment_column, segment_row)
        for h in range(local_heads):
            scores = dot_nt(qkv[rows, h * HD : (h + 1) * HD], keys) * scale
            scores = jnp.where(mask, scores, NEG_FILL)
            top = jnp.max(scores, axis=-1, keepdims=True)
            expon = jnp.exp(scores - top)
            total = jnp.sum(expon, axis=-1, keepdims=True)
            probs = (expon / total).astype(BF16)
            attn[rows, h * HD : (h + 1) * HD] = dot(probs, values, BF16)
            stats[rows, h * LANES : (h + 1) * LANES] = jnp.broadcast_to(
                top + jnp.log(total), (ROW_BLOCK, LANES)
            )
        both = dot_nt(attn[rows, :], w_o_here[...])
        mid = both[:, -LANES:].astype(BF16)
        mid_o[rows, :] = mid
        share[rows, :] = (both[:, :-LANES] + dot(mid, leave[...])).astype(BF16)


def attention_forward(normed, enter, leave, gains, cosine, sine, segments, qkv_parts, o_parts, scale):
    w_qkv, w_o = qkv_parts[0], o_parts[0]
    length, width = normed.shape
    columns = w_qkv.shape[1]
    local_heads = columns // HD - 2
    shapes = [
        ((length, columns - HD), F32), ((length, columns), BF16), ((length, local_heads * HD), BF16),
        ((length, LANES), BF16), ((length, LANES), BF16), ((length, local_heads * LANES), F32),
        ((length, width), BF16),
    ]
    vmem = pl.BlockSpec(memory_space=pltpu.VMEM)
    return pl.pallas_call(
        functools.partial(attention_forward_kernel, local_heads, scale),
        out_shape=[jax.ShapeDtypeStruct(*shape) for shape in shapes],
        in_specs=[vmem] * 8 + [pl.BlockSpec(memory_space=pl.ANY)] * 4,
        out_specs=[vmem] * len(shapes),
        scratch_shapes=[
            with_slots(w_qkv), with_slots(w_o), pltpu.SemaphoreType.DMA((2, 2)),
        ],
        name="attention_forward",
    )(normed, enter, leave, gains, cosine, sine, segments[:, None], segments[None, :], w_qkv, w_o,
        qkv_parts[1], o_parts[1])


def fold_rows(wide):
    row = lax.broadcasted_iota(jnp.int32, wide.shape, 0)
    lane = lax.broadcasted_iota(jnp.int32, wide.shape, 1)
    kept = jnp.where((lane % LANES) // RANK == row % GROUPS, wide, 0.0)
    return jnp.sum(kept.reshape(wide.shape[0] // GROUPS, GROUPS, wide.shape[1]), axis=1).astype(BF16)


def attention_backward_kernel(
    local_heads, scale, grad_branch, enter, leave, gains, cosine, sine, segment_column, segment_row,
    spread, raw, qkv, attn, stats, normed, mid_qkv, mid_o, w_qkv, w_o, s_qkv, s_o,
    share, entry_qkv, entry_o, exit_qkv, exit_o,
    w_qkv_here, w_o_here, grad_attn, grad_raw, grad_k, grad_v, spread_qkv, spread_o, sems,
):
    copies = [
        weight_copies((w_o, s_o), w_o_here, sems.at[0]),
        weight_copies((w_qkv, s_qkv), w_qkv_here, sems.at[1]),
    ]
    for c in copies[0] + copies[1]:
        c.start()
    blocks = normed.shape[0] // ROW_BLOCK
    key_col = local_heads * HD
    value_col = key_col + HD
    grad_k[...] = jnp.zeros_like(grad_k)
    grad_v[...] = jnp.zeros_like(grad_v)
    for c in copies[0]:
        c.wait()

    @pl.loop(0, blocks)
    def _(i):
        rows = rows_at(i)
        g = grad_branch[rows, :]
        mid = dot_nt(g, leave[...], BF16)
        spread_o[rows, :] = dot(mid, spread[:, :LANES], BF16)
        grad_attn[rows, :] = dot(jnp.concatenate([g, mid], axis=1), w_o_here[...], BF16)

    @pl.loop(0, blocks)
    def _(i):
        rows = rows_at(i)
        first = key_start(i)
        span = pl.ds(first, KEY_SPAN)
        keys = qkv[span, key_col:value_col]
        values = qkv[span, value_col:]
        mask = allowed_keys(i, first, segment_column, segment_row)
        for h in range(local_heads):
            columns = slice(h * HD, (h + 1) * HD)
            q = qkv[rows, columns]
            g = grad_attn[rows, columns]
            scores = jnp.where(mask, dot_nt(q, keys) * scale, NEG_FILL)
            probs = jnp.exp(scores - stats[rows, h * LANES : h * LANES + 1])
            grad_probs = dot_nt(g, values)
            inner = jnp.sum(probs * grad_probs, axis=-1, keepdims=True)
            grad_scores = (probs * (grad_probs - inner)).astype(BF16)
            grad_q = dot(grad_scores, keys) * scale
            grad_k[span, :] += dot_tn(grad_scores, q) * scale
            grad_v[span, :] += dot_tn(probs.astype(BF16), g)
            grad_raw[rows, columns] = head_backward(
                raw[rows, columns], gains[0:1, :], cosine[rows, :], sine[rows, :], grad_q
            ).astype(BF16)

    for c in copies[1]:
        c.wait()

    @pl.loop(0, blocks)
    def _(i):
        rows = rows_at(i)
        grad_raw[rows, key_col:value_col] = head_backward(
            raw[rows, key_col:value_col], gains[1:2, :], cosine[rows, :], sine[rows, :], grad_k[rows, :]
        ).astype(BF16)
        grad_raw[rows, value_col:] = grad_v[rows, :].astype(BF16)
        both = dot_nt(grad_raw[rows, :], w_qkv_here[...])
        mid = both[:, -LANES:].astype(BF16)
        spread_qkv[rows, :] = dot(mid, spread[...], BF16)
        share[rows, :] = (both[:, :-LANES] + dot_nt(mid, enter[...])).astype(BF16)

    @pl.loop(0, normed.shape[1] // LANES)
    def _(j):
        wide = dot_tn(normed[:, rows_at(j, LANES)], spread_qkv[...])
        entry_qkv[rows_at(j, RANK), :] = fold_rows(wide)

    @pl.loop(0, attn.shape[1] // LANES)
    def _(j):
        wide = dot_tn(attn[:, rows_at(j, LANES)], spread_o[...])
        entry_o[rows_at(j, RANK), :] = fold_rows(wide)

    exits = (ADAPTER_SCALING * dot_tn(mid_qkv[...], grad_raw[...])).astype(BF16)
    exit_qkv[:, :key_col] = exits[:RANK, :key_col]
    exit_qkv[:, key_col:value_col] = exits[RANK : 2 * RANK, key_col:value_col]
    exit_qkv[:, value_col:] = exits[2 * RANK : 3 * RANK, value_col:]
    exit_o[...] = (ADAPTER_SCALING * dot_tn(mid_o[...], grad_branch[...]))[:RANK].astype(BF16)


def attention_backward(
    grad_branch, enter, leave, gains, cosine, sine, segments, kept, qkv_parts, o_parts, scale
):
    w_qkv, w_o = qkv_parts[0], o_parts[0]
    length, width = grad_branch.shape
    columns = w_qkv.shape[1]
    local_heads = columns // HD - 2
    spread = jnp.concatenate([slot_spread(i) for i in range(3)], axis=1)
    shapes = [
        (length, width), (width // GROUPS, 3 * LANES), (local_heads * HD // GROUPS, LANES),
        (RANK, columns), (RANK, width),
    ]
    vmem = pl.BlockSpec(memory_space=pltpu.VMEM)
    return pl.pallas_call(
        functools.partial(attention_backward_kernel, local_heads, scale),
        out_shape=[jax.ShapeDtypeStruct(shape, BF16) for shape in shapes],
        in_specs=[vmem] * 16 + [pl.BlockSpec(memory_space=pl.ANY)] * 4,
        out_specs=[vmem] * len(shapes),
        scratch_shapes=[
            with_slots(w_qkv), with_slots(w_o),
            pltpu.VMEM((length, local_heads * HD), BF16), pltpu.VMEM((length, columns), BF16),
            pltpu.VMEM((length, HD), F32), pltpu.VMEM((length, HD), F32),
            pltpu.VMEM((length, 3 * LANES), BF16), pltpu.VMEM((length, LANES), BF16),
            pltpu.SemaphoreType.DMA((2, 2)),
        ],
        name="attention_backward",
    )(
        grad_branch, enter, leave, gains, cosine, sine, segments[:, None], segments[None, :], spread,
        kept["raw"], kept["qkv"], kept["attn"], kept["stats"], kept["normed"], kept["mid_qkv"],
        kept["mid_o"], w_qkv, w_o, qkv_parts[1], o_parts[1],
    )


def gelu_parts(v):
    c = math.sqrt(2.0 / math.pi)
    th = jnp.tanh(c * (v + 0.044715 * v * v * v))
    value = 0.5 * v * (1.0 + th)
    slope = 0.5 * (1.0 + th) + 0.5 * v * (1.0 - th * th) * (c * (1.0 + 3.0 * 0.044715 * v * v))
    return value, slope


FFN_BLOCK = 1152


def ffn_fetch(weights, offsets, buffers, sems, j, slot):
    out = []
    for k in range(3):
        source, slots = weights[2 * k], weights[2 * k + 1]
        here = buffers.at[k, slot]
        start = pl.multiple_of(j * FFN_BLOCK, LANES)
        rows = source.shape[0]
        out.append(pltpu.make_async_copy(
            source.at[:, pl.ds(offsets[k] + start, FFN_BLOCK)], here.at[pl.ds(0, rows)], sems.at[k, slot, 0]
        ))
        out.append(pltpu.make_async_copy(
            slots.at[:, pl.ds(start, FFN_BLOCK)], here.at[pl.ds(rows, LANES)], sems.at[k, slot, 1]
        ))
    return out


def ffn_step(weights, offsets, buffers, sems, steps):
    j = pl.program_id(0)
    slot = j % 2

    @pl.when(j == 0)
    def _():
        for c in ffn_fetch(weights, offsets, buffers, sems, 0, 0):
            c.start()

    for c in ffn_fetch(weights, offsets, buffers, sems, j, slot):
        c.wait()

    @pl.when(j + 1 < steps)
    def _():
        for c in ffn_fetch(weights, offsets, buffers, sems, j + 1, 1 - slot):
            c.start()

    return slot


def ffn_forward_kernel(
    offsets, steps, z, enter, leave, w_g, s_g, w_u, s_u, w_d, s_d,
    gelu, slope, hidden, mid_gu, mid_d, share, buffers, joined, total, sems,
):
    j = pl.program_id(0)
    width = z.shape[1]
    blocks = z.shape[0] // ROW_BLOCK
    slot = ffn_step((w_g, s_g, w_u, s_u, w_d, s_d), offsets, buffers, sems, steps)

    @pl.when(j == 0)
    def _():
        mid = dot(z[...], enter[...], BF16)
        mid_gu[...] = mid
        joined[:, :width] = z[...]
        joined[:, width:] = mid

    @pl.loop(0, blocks)
    def _(i):
        rows = rows_at(i)
        gate_pre = dot(joined[rows, :], buffers[0, slot])
        up_pre = dot(joined[rows, :], buffers[1, slot])
        value, rate = gelu_parts(gate_pre)
        gelu[rows, :] = value.astype(BF16)
        slope[rows, :] = (rate * up_pre).astype(BF16)
        hidden[rows, :] = (value * up_pre).astype(BF16)

    part = dot_nt(hidden[...], buffers[2, slot])

    @pl.when(j == 0)
    def _():
        total[...] = part

    @pl.when(j > 0)
    def _():
        total[...] += part

    @pl.when(j == steps - 1)
    def _():
        mid = total[:, width:].astype(BF16)
        mid_d[...] = mid
        share[...] = (total[:, :width] + dot(mid, leave[...])).astype(BF16)


def ffn_forward(z, enter, leave, weights, offsets):
    length, width = z.shape
    columns = weights[1].shape[1]
    steps = columns // FFN_BLOCK

    def fixed(shape):
        return pl.BlockSpec(shape, lambda j: (0, 0), pipeline_mode=pl.Buffered(1))

    wide = pl.BlockSpec((length, FFN_BLOCK), lambda j: (0, j))
    hbm = pl.BlockSpec(memory_space=pl.ANY)
    small = (length, LANES)
    return pl.pallas_call(
        functools.partial(ffn_forward_kernel, offsets, steps),
        grid=(steps,),
        out_shape=[jax.ShapeDtypeStruct((length, columns), BF16)] * 3
        + [jax.ShapeDtypeStruct(small, BF16)] * 2
        + [jax.ShapeDtypeStruct((length, width), BF16)],
        in_specs=[fixed(z.shape), fixed(enter.shape), fixed(leave.shape)] + [hbm] * 6,
        out_specs=[wide] * 3 + [fixed(small), fixed(small), fixed((length, width))],
        scratch_shapes=[
            pltpu.VMEM((3, 2, width + LANES, FFN_BLOCK), BF16),
            pltpu.VMEM((length, width + LANES), BF16),
            pltpu.VMEM((length, width + LANES), F32),
            pltpu.SemaphoreType.DMA((3, 2, 2)),
        ],
        compiler_params=pltpu.CompilerParams(vmem_limit_bytes=VMEM_LIMIT),
        name="ffn_forward",
    )(z, enter, leave, *weights)


def ffn_backward_kernel(
    offsets, steps, grad, z, enter, leave, mid_gu, mid_d, spread, gelu, slope, hidden,
    w_g, s_g, w_u, s_u, w_d, s_d,
    share, exit_g, exit_u, entry_d, exit_d, entry_gu,
    buffers, joined, grad_g, grad_u, total, spread_d, spread_gu, sems,
):
    j = pl.program_id(0)
    width = z.shape[1]
    blocks = z.shape[0] // ROW_BLOCK
    slot = ffn_step((w_g, s_g, w_u, s_u, w_d, s_d), offsets, buffers, sems, steps)

    @pl.when(j == 0)
    def _():
        mid = dot_nt(grad[...], leave[...], BF16)
        joined[:, :width] = grad[...]
        joined[:, width:] = mid
        spread_d[...] = dot(mid, spread[:, :LANES], BF16)
        exit_d[...] = (ADAPTER_SCALING * dot_tn(mid_d[...], grad[...]))[:RANK].astype(BF16)

    @pl.loop(0, blocks)
    def _(i):
        rows = rows_at(i)
        grad_hidden = dot(joined[rows, :], buffers[2, slot])
        grad_g[rows, :] = (grad_hidden * slope[rows, :].astype(F32)).astype(BF16)
        grad_u[rows, :] = (grad_hidden * gelu[rows, :].astype(F32)).astype(BF16)

    part = dot_nt(grad_g[...], buffers[0, slot]) + dot_nt(grad_u[...], buffers[1, slot])

    @pl.when(j == 0)
    def _():
        total[...] = part

    @pl.when(j > 0)
    def _():
        total[...] += part

    exit_g[...] = (ADAPTER_SCALING * dot_tn(mid_gu[...], grad_g[...]))[:RANK].astype(BF16)
    exit_u[...] = (ADAPTER_SCALING * dot_tn(mid_gu[...], grad_u[...]))[RANK : 2 * RANK].astype(BF16)

    @pl.loop(0, FFN_BLOCK // LANES)
    def _(i):
        wide = dot_tn(hidden[:, rows_at(i, LANES)], spread_d[...])
        entry_d[rows_at(i, RANK), :] = fold_rows(wide)

    @pl.when(j == steps - 1)
    def _():
        mid = total[:, width:].astype(BF16)
        share[...] = (total[:, :width] + dot_nt(mid, enter[...])).astype(BF16)
        spread_gu[...] = dot(mid, spread[...], BF16)

        @pl.loop(0, width // LANES)
        def _(i):
            wide = dot_tn(z[:, rows_at(i, LANES)], spread_gu[...])
            entry_gu[rows_at(i, RANK), :] = fold_rows(wide)


def ffn_backward(grad, z, enter, leave, kept, weights, offsets):
    length, width = z.shape
    columns = weights[1].shape[1]
    steps = columns // FFN_BLOCK
    spread = jnp.concatenate([slot_spread(i) for i in range(2)], axis=1)

    def fixed(shape):
        return pl.BlockSpec(shape, lambda j: (0, 0), pipeline_mode=pl.Buffered(1))

    wide = pl.BlockSpec((length, FFN_BLOCK), lambda j: (0, j))
    hbm = pl.BlockSpec(memory_space=pl.ANY)
    small = (length, LANES)
    shapes = [
        (length, width), (RANK, columns), (RANK, columns), (columns // GROUPS, LANES), (RANK, width),
        (width // GROUPS, 2 * LANES),
    ]
    narrow = pl.BlockSpec((RANK, FFN_BLOCK), lambda j: (0, j))
    return pl.pallas_call(
        functools.partial(ffn_backward_kernel, offsets, steps),
        grid=(steps,),
        out_shape=[jax.ShapeDtypeStruct(shape, BF16) for shape in shapes],
        in_specs=[
            fixed(grad.shape), fixed(z.shape), fixed(enter.shape), fixed(leave.shape), fixed(small),
            fixed(small), fixed(spread.shape), wide, wide, wide,
        ] + [hbm] * 6,
        out_specs=[
            fixed((length, width)), narrow, narrow,
            pl.BlockSpec((FFN_BLOCK // GROUPS, LANES), lambda j: (j, 0)),
            fixed((RANK, width)), fixed((width // GROUPS, 2 * LANES)),
        ],
        scratch_shapes=[
            pltpu.VMEM((3, 2, width + LANES, FFN_BLOCK), BF16),
            pltpu.VMEM((length, width + LANES), BF16),
            pltpu.VMEM((length, FFN_BLOCK), BF16),
            pltpu.VMEM((length, FFN_BLOCK), BF16),
            pltpu.VMEM((length, width + LANES), F32),
            pltpu.VMEM(small, BF16),
            pltpu.VMEM((length, 2 * LANES), BF16),
            pltpu.SemaphoreType.DMA((3, 2, 2)),
        ],
        compiler_params=pltpu.CompilerParams(vmem_limit_bytes=VMEM_LIMIT),
        name="ffn_backward",
    )(
        grad, z, enter, leave, kept["mid_gu"], kept["mid_d"], spread, kept["gelu"], kept["slope"],
        kept["hidden"], *weights,
    )


def shards(
    hidden_in, out_grad, segments, positions, set_ids, query_w, key_w, value_w, out_w, gate_w,
    up_w, down_w, norm_gains, head_gains, adapters, first_moment, second_moment,
):
    tp_count = lax.axis_size("tp")
    fsdp_count = lax.axis_size("fsdp")
    tp_place = lax.axis_index("tp")
    set_count, share = adapters.shape
    head_cols = HEADS * HD // tp_count
    hidden_cols = FF // tp_count
    scale = HD ** (-0.5)
    set_range = jnp.arange(set_count, dtype=jnp.int32)

    master_low = adapters.astype(BF16)
    owner_sets = jnp.repeat(set_ids, tp_count)
    selector = (owner_sets[:, None] == set_range[None, :]).astype(BF16)
    routed = dot(selector, master_low, BF16)
    whole_rows = share % LANES == 0
    if whole_rows:
        routed = routed.reshape(-1, share // LANES, LANES)
    own = lax.all_to_all(routed, ("fsdp", "tp"), split_axis=0, concat_axis=0, tiled=True)

    def local_weights(l):
        return {
            "qkv": jnp.concatenate([query_w[l], key_w[l], value_w[l]], axis=1),
            "o": out_w[l].T,
            "g": gate_w[l],
            "u": up_w[l],
            "d": down_w[l].T,
        }

    local = [local_weights(l) for l in range(LAYERS)]
    first_names = [(0, "qkv"), (0, "o"), (0, "g"), (0, "u"), (0, "d"), (1, "qkv"), (1, "o"), (1, "g")]
    late = jnp.concatenate([local[1]["u"], local[1]["d"]], axis=1)
    arrays = [local[l][name] for l, name in first_names]
    if fsdp_count == 16:
        part = hidden_cols * 4 // 9 // LANES * LANES
        plan = [
            ("zxy", 0, (0, arrays[0].shape[1])), ("zxy", 1, (0, arrays[1].shape[1])),
            ("zyx", 5, (0, arrays[5].shape[1])), ("zyx", 6, (0, arrays[6].shape[1])),
            ("zxy", 2, (0, hidden_cols)), ("zyx", 3, (0, hidden_cols)),
            ("xyz", 4, (part, hidden_cols - part)), ("yxz", 7, (part, hidden_cols - part)),
            ("zxy", 4, (0, part)), ("zyx", 7, (0, part)),
        ]
        first = gather_weights(arrays, plan, fsdp_count, 11)
    else:
        first = [lax.all_gather(a, "fsdp", axis=0, tiled=True) for a in arrays]
    own, late, first = lax.optimization_barrier((own, late, first))
    late_all = lax.all_gather(late, "fsdp", axis=0, tiled=True)

    if whole_rows:
        own_rows = own.reshape(-1, LANES)
    else:
        own_rows = own.reshape(-1).reshape(-1, LANES)
    layer_rows = sum(n for _, n in PIECES) * RANK // LANES

    def unpack(l):
        at = l * layer_rows
        got = {}
        for name, n in PIECES:
            count = n * RANK // LANES
            rows = own_rows[at : at + count]
            at += count
            if name in ("Eo", "Ed"):
                rows = lax.dynamic_slice_in_dim(rows, tp_place * (count // tp_count), count // tp_count, 0)
            if name[0] == "X":
                if name in ("Xq", "Xg", "Xu"):
                    parts = n // LANES
                    rows = rows.reshape(RANK, parts, LANES)
                    rows = lax.dynamic_slice_in_dim(
                        rows, tp_place * (parts // tp_count), parts // tp_count, 1
                    )
                got[name] = rows.reshape(RANK, -1)
            else:
                got[name] = expand_entry(rows)
        return got

    maps, spares = [], []
    for l in range(LAYERS):
        m = unpack(l)
        m["enter_qkv"] = dot(
            jnp.concatenate([m["Eq"], m["Ek"], m["Ev"]], axis=1),
            jnp.concatenate([slot_pick(i) for i in range(3)], axis=0), BF16,
        )
        m["enter_gu"] = dot(
            jnp.concatenate([m["Eg"], m["Eu"]], axis=1),
            jnp.concatenate([slot_pick(i) for i in range(2)], axis=0), BF16,
        )
        m["leave_o"] = in_slot(ADAPTER_SCALING * m["Xo"], 0)
        m["leave_d"] = in_slot(ADAPTER_SCALING * m["Xd"], 0)
        spares.append({
            "qkv": ADAPTER_SCALING * jnp.concatenate(
                [in_slot(m["Xq"], 0), in_slot(m["Xk"], 1), in_slot(m["Xv"], 2)], axis=1
            ),
            "o": dot_tn(slot_pick(0), m["Eo"].T, BF16),
            "g": ADAPTER_SCALING * in_slot(m["Xg"], 0),
            "u": ADAPTER_SCALING * in_slot(m["Xu"], 1),
            "d": dot_tn(slot_pick(0), m["Ed"].T, BF16),
        })
        maps.append(m)

    weights = [dict(), dict()]
    for (l, name), array in zip(first_names, first):
        weights[l][name] = (array, spares[l][name].astype(BF16))
    weights[1]["u"] = (late_all, spares[1]["u"].astype(BF16))
    weights[1]["d"] = (late_all, spares[1]["d"].astype(BF16))
    ffn_weights = [w["g"] + w["u"] + w["d"] for w in weights]
    ffn_offsets = [(0, 0, 0), (0, 0, hidden_cols)]
    cosine, sine = rope_tables(positions)
    gains = norm_gains.astype(F32)
    heads = head_gains.astype(F32)

    def gain(l, i):
        return gains[l, i][None, :]

    kept = []
    normed = exchange(body_enter, 1, "enter", None, [hidden_in], [gain(0, 0)], [], True)[0]
    x = hidden_in
    for l in range(LAYERS):
        w = weights[l]
        r = {"x": x, "normed": normed}
        m = maps[l]
        (
            r["raw"], r["qkv"], r["attn"], r["mid_qkv"], r["mid_o"], r["stats"], share_o,
        ) = attention_forward(
            normed, m["enter_qkv"], m["leave_o"], heads[l], cosine, sine, segments, w["qkv"],
            w["o"], scale,
        )
        r["attn_branch"], r["middle"], r["normed_two"] = exchange(
            body_middle, 2 if l == 0 else 3, "middle", share_o, [x], [gain(l, 1), gain(l, 2)],
            [F32, F32], True,
        )
        r["gelu"], r["slope"], r["hidden"], r["mid_gu"], r["mid_d"], share_f = ffn_forward(
            r["normed_two"], m["enter_gu"], m["leave_d"], ffn_weights[l], ffn_offsets[l]
        )
        if l + 1 < LAYERS:
            r["ffn_branch"], x, normed = exchange(
                body_next, 4, "next", share_f, [r["middle"]], [gain(l, 3), gain(l + 1, 0)],
                [F32, F32], True,
            )
        else:
            result, grad_ffn = exchange(
                body_turn, 5, "turn", share_f, [r["middle"], out_grad], [gain(l, 3)], [BF16], True
            )
        kept.append(r)

    grad_out = out_grad
    layer_grads = [None] * LAYERS
    for l in reversed(range(LAYERS)):
        w, r, m = weights[l], kept[l], maps[l]
        pieces = {}

        share_n2, pieces["Xg"], pieces["Xu"], pieces["Ed"], pieces["Xd"], entry_gu = ffn_backward(
            grad_ffn, r["normed_two"], m["enter_gu"], m["leave_d"], r, ffn_weights[l], ffn_offsets[l]
        )
        pieces["Eg"], pieces["Eu"] = entry_gu[:, :LANES], entry_gu[:, LANES:]
        grad_middle, grad_branch = exchange(
            body_back_middle, 6 if l == 1 else 7, "back_middle", share_n2,
            [grad_out, r["middle"], r["attn_branch"]], [gain(l, 2), gain(l, 1)], [F32], True,
        )
        share_n, entry_qkv, pieces["Eo"], exit_qkv, pieces["Xo"] = attention_backward(
            grad_branch, m["enter_qkv"], m["leave_o"], heads[l], cosine, sine, segments, r, w["qkv"],
            w["o"], scale,
        )
        for i, name in enumerate("qkv"):
            pieces["E" + name] = entry_qkv[:, i * LANES : (i + 1) * LANES]
        pieces["Xq"] = exit_qkv[:, :head_cols]
        pieces["Xk"] = exit_qkv[:, head_cols : head_cols + HD]
        pieces["Xv"] = exit_qkv[:, head_cols + HD :]
        if l > 0:
            grad_out, grad_ffn = exchange(
                body_back_next, 8, "back_next", share_n,
                [grad_middle, r["x"], kept[l - 1]["ffn_branch"]], [gain(l, 0), gain(l - 1, 3)],
                [F32], True,
            )
        else:
            grad_out = exchange(
                body_back_last, 9, "back_last", share_n, [grad_middle, r["x"]], [gain(l, 0)], [F32], False
            )[0]
        rows = []
        for name, n in PIECES:
            piece = pieces[name]
            if name in ("Eo", "Ed"):
                piece = lax.dynamic_update_slice_in_dim(
                    jnp.zeros((n * RANK // LANES, LANES), BF16), piece, tp_place * piece.shape[0], 0
                )
            if name in ("Xq", "Xg", "Xu"):
                piece = lax.dynamic_update_slice_in_dim(
                    jnp.zeros((RANK, n), BF16), piece, tp_place * piece.shape[1], 1
                )
            rows.append(piece.reshape(-1, LANES))
        layer_grads[l] = rows

    flat = jnp.concatenate(layer_grads[0] + layer_grads[1], axis=0)
    if whole_rows:
        flat = flat.reshape(fsdp_count * tp_count, share // LANES, LANES)
    else:
        flat = flat.reshape(-1).reshape(fsdp_count * tp_count, 1, share)
    chip_sum = pair_sum(flat, 10)
    arrived = lax.all_to_all(chip_sum, "fsdp", split_axis=0, concat_axis=0, tiled=True).reshape(fsdp_count, share)
    owner_pick = (set_range[:, None] == set_ids[None, :]).astype(BF16)
    set_grads = dot(owner_pick, arrived)
    first_new = BETA_ONE * first_moment + (1.0 - BETA_ONE) * set_grads
    second_new = BETA_TWO * second_moment + (1.0 - BETA_TWO) * set_grads * set_grads
    first_hat = first_new / (1.0 - BETA_ONE**ADAM_STEPS)
    second_hat = second_new / (1.0 - BETA_TWO**ADAM_STEPS)
    new_master = adapters - LEARN_RATE * (
        first_hat / (jnp.sqrt(second_hat) + ADAM_EPS) + DECAY_RATE * adapters
    )
    return (
        result, grad_out, set_grads, new_master, first_new, second_new, new_master.astype(BF16),
    )


def solution(mesh):
    return jax.shard_map(
        shards,
        mesh=mesh,
        in_specs=(
            P(("fsdp", "tp"), None),
            P(("fsdp", "tp"), None),
            P("fsdp"),
            P("fsdp"),
            P(),
            P(None, "fsdp", "tp"),
            P(None, "fsdp", None),
            P(None, "fsdp", None),
            P(None, "tp", "fsdp"),
            P(None, "fsdp", "tp"),
            P(None, "fsdp", "tp"),
            P(None, "tp", "fsdp"),
            P(),
            P(),
            P(None, ("fsdp", "tp")),
            P(None, ("fsdp", "tp")),
            P(None, ("fsdp", "tp")),
        ),
        out_specs=(
            P(("fsdp", "tp"), None),
            P(("fsdp", "tp"), None),
            P(None, ("fsdp", "tp")),
            P(None, ("fsdp", "tp")),
            P(None, ("fsdp", "tp")),
            P(None, ("fsdp", "tp")),
            P(None, ("fsdp", "tp")),
        ),
        check_vma=False,
    )
```

```python
import functools
import math

import jax
import jax.numpy as jnp
from jax import lax
from jax.experimental import pallas as pl
from jax.experimental.pallas import tpu as pltpu
from jax.sharding import PartitionSpec as P

D = 1152
HEADS = 4
HD = 256
FF = 6912
WINDOW = 512
RANK = 16
LAYERS = 2
LANES = 128
GROUPS = LANES // RANK

NORM_EPS = 1e-06
ADAPTER_SCALING = 4.0
ROPE_BASE = 10000.0
LEARN_RATE = 0.01
BETA_ONE = 0.5
BETA_TWO = 0.6
ADAM_STEPS = 4.0
ADAM_EPS = 1e-08
DECAY_RATE = 0.1
NEG_FILL = -1e30
F32 = jnp.float32
BF16 = jnp.bfloat16
MESH = pl.DeviceIdType.MESH
EXCHANGE_CHUNKS = 8

PIECES = (
    ("Eq", D), ("Xq", HEADS * HD), ("Ek", D), ("Xk", HD), ("Ev", D), ("Xv", HD),
    ("Eo", HEADS * HD), ("Xo", D), ("Eg", D), ("Xg", FF), ("Eu", D), ("Xu", FF),
    ("Ed", FF), ("Xd", D),
)


def dot(a, b, out=F32):
    return lax.dot_general(a, b, (((1,), (0,)), ((), ())), preferred_element_type=F32).astype(out)


def dot_nt(a, b, out=F32):
    return lax.dot_general(a, b, (((1,), (1,)), ((), ())), preferred_element_type=F32).astype(out)


def dot_tn(a, b, out=F32):
    return lax.dot_general(a, b, (((0,), (0,)), ((), ())), preferred_element_type=F32).astype(out)


def rms(v, gain):
    return v * lax.rsqrt(jnp.mean(v * v, axis=-1, keepdims=True) + NORM_EPS) * (1.0 + gain)


def rms_back(v, gain, dy):
    r = lax.rsqrt(jnp.mean(v * v, axis=-1, keepdims=True) + NORM_EPS)
    scaled = (1.0 + gain) * dy
    return r * scaled - v * (r * r * r) * jnp.mean(v * scaled, axis=-1, keepdims=True)


def exchange_kernel(body, has_partial, n_rows, n_gains, n_outs, has_send, n_chunks, *refs):
    refs = list(refs)

    def take(count):
        out = refs[:count]
        del refs[:count]
        return out

    partial = take(1)[0] if has_partial else None
    rows, gains, outs = take(n_rows), take(n_gains), take(n_outs)
    gathered = take(1)[0] if has_send else None
    rows_here, outs_here = take(n_rows), take(n_outs)
    row_sems, out_sems = take(2)
    if has_partial:
        mine, arrived, mine_sems, send_a, recv_a = take(5)
    if has_send:
        spread_here, keep_sems, send_b, recv_b = take(4)
    me = lax.axis_index("tp")
    other = 1 - me
    half = (partial if has_partial else gathered).shape[0] // 2
    chunk = half // n_chunks

    def span(base, c):
        return pl.ds(pl.multiple_of(base * half + c * chunk, chunk), chunk)

    def local(c):
        return pl.ds(c * chunk, chunk)

    loads = []
    for c in range(n_chunks):
        group = [
            pltpu.make_async_copy(r.at[local(c)], h.at[local(c)], row_sems.at[i, c])
            for i, (r, h) in enumerate(zip(rows, rows_here))
        ]
        if has_partial:
            group.append(
                pltpu.make_async_copy(partial.at[span(me, c)], mine.at[local(c)], mine_sems.at[c])
            )
        for copy in group:
            copy.start()
        loads.append(group)
    barrier = pltpu.get_barrier_semaphore()
    pl.semaphore_signal(barrier, inc=1, device_id={"tp": other}, device_id_type=MESH)
    pl.semaphore_wait(barrier, 1)
    sends, spreads, stores = [], [], []
    if has_partial:
        for c in range(n_chunks):
            copy = pltpu.make_async_remote_copy(
                src_ref=partial.at[span(other, c)],
                dst_ref=arrived.at[local(c)],
                send_sem=send_a.at[c],
                recv_sem=recv_a.at[c],
                device_id={"tp": other},
                device_id_type=MESH,
            )
            copy.start()
            sends.append(copy)
    gain_values = [g[...].astype(F32) for g in gains]

    def release(c):
        if has_send:
            spreads[c].start()
        for copy in stores[c]:
            copy.start()

    for c in range(n_chunks):
        for copy in loads[c]:
            copy.wait()
        total = None
        if has_partial:
            sends[c].wait_recv()
            total = mine[local(c), :].astype(F32) + arrived[local(c), :].astype(F32)
        values, spread = body(total, [r[local(c), :].astype(F32) for r in rows_here], gain_values)
        group = []
        for i, (ref, here, value) in enumerate(zip(outs, outs_here, values)):
            here[local(c), :] = value.astype(here.dtype)
            group.append(pltpu.make_async_copy(here.at[local(c)], ref.at[local(c)], out_sems.at[i, c]))
        if has_send:
            spread_here[local(c), :] = spread.astype(BF16)
            group.append(
                pltpu.make_async_copy(spread_here.at[local(c)], gathered.at[span(me, c)], keep_sems.at[c])
            )
            spreads.append(
                pltpu.make_async_remote_copy(
                    src_ref=spread_here.at[local(c)],
                    dst_ref=gathered.at[span(me, c)],
                    send_sem=send_b.at[c],
                    recv_sem=recv_b.at[c],
                    device_id={"tp": other},
                    device_id_type=MESH,
                )
            )
        stores.append(group)
        if c > 0:
            release(c - 1)
    release(n_chunks - 1)
    for copy in sends:
        copy.wait_send()
    for c in range(n_chunks):
        for copy in stores[c]:
            copy.wait()
    for copy in spreads:
        copy.wait()


def exchange(body, collective_id, name, partial, rows, gains, out_types, has_send, n_chunks=EXCHANGE_CHUNKS):
    operands = ([] if partial is None else [partial]) + list(rows)
    width = operands[0].shape[1]
    half = partial.shape[0] // 2 if partial is not None else rows[0].shape[0]
    outs = [jax.ShapeDtypeStruct((half, width), kind) for kind in out_types]
    scratch = [pltpu.VMEM((half, width), r.dtype) for r in rows]
    scratch += [pltpu.VMEM((half, width), kind) for kind in out_types]
    scratch += [
        pltpu.SemaphoreType.DMA((len(rows), n_chunks)),
        pltpu.SemaphoreType.DMA((max(len(outs), 1), n_chunks)),
    ]
    each = pltpu.SemaphoreType.DMA((n_chunks,))
    if partial is not None:
        scratch += [pltpu.VMEM((half, width), partial.dtype)] * 2 + [each] * 3
    if has_send:
        outs.append(jax.ShapeDtypeStruct((2 * half, width), BF16))
        scratch += [pltpu.VMEM((half, width), BF16)] + [each] * 3
    hbm = pl.BlockSpec(memory_space=pl.ANY)
    return pl.pallas_call(
        functools.partial(
            exchange_kernel, body, partial is not None, len(rows), len(gains), len(out_types),
            has_send, n_chunks,
        ),
        out_shape=outs,
        in_specs=[hbm] * len(operands) + [pl.BlockSpec(memory_space=pltpu.VMEM)] * len(gains),
        out_specs=[hbm] * len(outs),
        scratch_shapes=scratch,
        compiler_params=pltpu.CompilerParams(collective_id=collective_id, has_side_effects=True),
        name=name,
    )(*operands, *gains)


def gather_kernel(plan, nz, rows, n_arrays, *refs):
    mine, gathered = refs[:n_arrays], refs[n_arrays : 2 * n_arrays]
    send_sem, recv_sem, local_sem = refs[2 * n_arrays :]
    f = lax.axis_index("fsdp")
    x, y, z = f % 2, (f // 2) % 2, f // 4

    def index(a, b, c):
        return (a * 2 + b) * 2 + c

    peers = {
        "x": (index(z, y, 1 - x), None),
        "y": (index(z, 1 - y, x), None),
        "u": (f + 4, z < nz - 1),
        "d": (f - 4, z > 0),
    }
    ways_index = "xyud".index

    def guarded(cond, fn):
        if cond is None:
            fn()
        else:
            pl.when(cond)(fn)

    barrier = pltpu.get_barrier_semaphore()

    def greet(peer):
        pl.semaphore_signal(barrier, inc=1, device_id={"fsdp": peer}, device_id_type=MESH)

    for peer, cond in peers.values():
        guarded(cond, functools.partial(greet, peer))
    inside = jnp.logical_and(z > 0, z < nz - 1)
    pl.when(inside)(lambda: pl.semaphore_wait(barrier, 4))
    pl.when(jnp.logical_not(inside))(lambda: pl.semaphore_wait(barrier, 3))

    offsets = [(dz, fy, fx) for dz in range(1 - nz, nz) for fy in (0, 1) for fx in (0, 1)]
    offsets.sort(key=lambda o: (abs(o[0]) + o[1] + o[2], o))
    ids = {o: i for i, o in enumerate(offsets)}
    own = (0, 0, 0)

    def place(array, source, columns):
        return gathered[array].at[pl.ds(pl.multiple_of(source * rows, 8), rows), pl.ds(*columns)]

    for a in range(n_arrays):
        pltpu.make_async_copy(
            mine[a], place(a, f, (0, mine[a].shape[1])), local_sem.at[a]
        ).start()

    def source_of(o):
        return index(z + o[0], y + o[1] - 2 * y * o[1], x + o[2] - 2 * x * o[2])

    def copy(k, o, way):
        target = {
            "u": (o[0] - 1, o[1], o[2]), "d": (o[0] + 1, o[1], o[2]),
            "x": (o[0], o[1], 1), "y": (o[0], 1, o[2]),
        }[way]
        _, array, columns = plan[k]
        block = place(array, source_of(o), columns)
        return pltpu.make_async_remote_copy(
            src_ref=mine[array].at[:, pl.ds(*columns)] if o == own else block,
            dst_ref=block,
            send_sem=send_sem.at[k, ids[o], ways_index(way)],
            recv_sem=recv_sem.at[k, ids[target]],
            device_id={"fsdp": peers[way][0]},
            device_id_type=MESH,
        )

    def arrival(k, o):
        _, array, columns = plan[k]
        block = place(array, source_of(o), columns)
        return pltpu.make_async_remote_copy(
            src_ref=block, dst_ref=block, send_sem=send_sem.at[k, ids[o], 0],
            recv_sem=recv_sem.at[k, ids[o]], device_id={"fsdp": peers["x"][0]}, device_id_type=MESH,
        )

    def ways(order, o):
        used = {"z": o[0] != 0, "y": o[1] != 0, "x": o[2] != 0}
        last = max([i for i, a in enumerate(order) if used[a]], default=-1)
        out = []
        if last >= 0 and order[last] == "z" and abs(o[0]) < nz - 1:
            out.append("d" if o[0] > 0 else "u")
        for a in order[last + 1 :]:
            out += ["u", "d"] if a == "z" else [a]
        return out

    def exists(o):
        if o[0] == 0:
            return None
        return z < nz - o[0] if o[0] > 0 else z >= -o[0]

    def pass_on(k, o):
        if o != own:
            arrival(k, o).wait_recv()
        for way in ways(plan[k][0], o):
            guarded(peers[way][1], lambda way=way: copy(k, o, way).start())

    def finish(k, o):
        for way in ways(plan[k][0], o):
            guarded(peers[way][1], lambda way=way: copy(k, o, way).wait_send())

    for step in (pass_on, finish):
        for o in offsets:
            for k in range(len(plan)):
                guarded(exists(o), functools.partial(step, k, o))
    for a in range(n_arrays):
        pltpu.make_async_copy(
            mine[a], place(a, f, (0, mine[a].shape[1])), local_sem.at[a]
        ).wait()


def gather_weights(arrays, plan, count, collective_id):
    rows = arrays[0].shape[0]
    nz = count // 4
    offsets = (2 * nz - 1) * 4
    return pl.pallas_call(
        functools.partial(gather_kernel, plan, nz, rows, len(arrays)),
        out_shape=[
            jax.ShapeDtypeStruct((count * rows, a.shape[1]), a.dtype) for a in arrays
        ],
        in_specs=[pl.BlockSpec(memory_space=pltpu.VMEM)] * len(arrays),
        out_specs=[pl.BlockSpec(memory_space=pl.ANY)] * len(arrays),
        scratch_shapes=[
            pltpu.SemaphoreType.DMA((len(plan), offsets, 4)),
            pltpu.SemaphoreType.DMA((len(plan), offsets)),
            pltpu.SemaphoreType.DMA((len(arrays),)),
        ],
        compiler_params=pltpu.CompilerParams(collective_id=collective_id, has_side_effects=True),
        name="gather_weights",
    )(*arrays)


def pair_sum_kernel(count, partial, total, arrived, send_sem, recv_sem):
    me = lax.axis_index("tp")
    other = 1 - me
    barrier = pltpu.get_barrier_semaphore()
    pl.semaphore_signal(barrier, inc=1, device_id={"tp": other}, device_id_type=MESH)
    pl.semaphore_wait(barrier, 1)
    copies = []
    for i in range(count):
        copy = pltpu.make_async_remote_copy(
            src_ref=partial.at[2 * i + other], dst_ref=arrived.at[i], send_sem=send_sem.at[i],
            recv_sem=recv_sem.at[i], device_id={"tp": other}, device_id_type=MESH,
        )
        copy.start()
        copies.append(copy)
    for i in range(count):
        copies[i].wait_recv()
        total[i] = (partial[2 * i + me].astype(F32) + arrived[i].astype(F32)).astype(total.dtype)
    for copy in copies:
        copy.wait_send()


def pair_sum(partial, collective_id):
    count = partial.shape[0] // 2
    shape = (count,) + partial.shape[1:]
    vmem = pl.BlockSpec(memory_space=pltpu.VMEM)
    return pl.pallas_call(
        functools.partial(pair_sum_kernel, count),
        out_shape=jax.ShapeDtypeStruct(shape, partial.dtype),
        in_specs=[vmem],
        out_specs=vmem,
        scratch_shapes=[
            pltpu.VMEM(shape, partial.dtype),
            pltpu.SemaphoreType.DMA((count,)),
            pltpu.SemaphoreType.DMA((count,)),
        ],
        compiler_params=pltpu.CompilerParams(collective_id=collective_id, has_side_effects=True),
        name="pair_sum",
    )(partial)


def pair_gather_kernel(count, mine, both, send_sem, recv_sem, local_sem):
    me = lax.axis_index("tp")
    other = 1 - me
    barrier = pltpu.get_barrier_semaphore()
    pl.semaphore_signal(barrier, inc=1, device_id={"tp": other}, device_id_type=MESH)
    pl.semaphore_wait(barrier, 1)
    copies = []
    for i in range(count):
        place = both.at[2 * i + me]
        copies.append(
            pltpu.make_async_remote_copy(
                src_ref=mine.at[i], dst_ref=place, send_sem=send_sem.at[i], recv_sem=recv_sem.at[i],
                device_id={"tp": other}, device_id_type=MESH,
            )
        )
        copies.append(pltpu.make_async_copy(mine.at[i], place, local_sem.at[i]))
    for copy in copies:
        copy.start()
    for copy in copies:
        copy.wait()


def pair_gather(mine, collective_id):
    count = mine.shape[0]
    return pl.pallas_call(
        functools.partial(pair_gather_kernel, count),
        out_shape=jax.ShapeDtypeStruct((2 * count,) + mine.shape[1:], mine.dtype),
        in_specs=[pl.BlockSpec(memory_space=pltpu.VMEM)],
        out_specs=pl.BlockSpec(memory_space=pl.ANY),
        scratch_shapes=[pltpu.SemaphoreType.DMA((count,))] * 3,
        compiler_params=pltpu.CompilerParams(collective_id=collective_id, has_side_effects=True),
        name="pair_gather",
    )(mine)


def body_enter(total, rows, gains):
    return [], rms(rows[0], gains[0])


def body_middle(total, rows, gains):
    middle = rows[0] + rms(total, gains[0])
    return [total, middle], rms(middle, gains[1])


def body_next(total, rows, gains):
    leaving = rows[0] + rms(total, gains[0])
    return [total, leaving], rms(leaving, gains[1])


def body_turn(total, rows, gains):
    leaving = rows[0] + rms(total, gains[0])
    return [leaving], rms_back(total, gains[0], rows[1])


def body_back_middle(total, rows, gains):
    grad_middle = rows[0] + rms_back(rows[1], gains[0], total)
    return [grad_middle], rms_back(rows[2], gains[1], grad_middle)


def body_back_next(total, rows, gains):
    grad_x = rows[0] + rms_back(rows[1], gains[0], total)
    return [grad_x], rms_back(rows[2], gains[1], grad_x)


def body_back_last(total, rows, gains):
    return [rows[0] + rms_back(rows[1], gains[0], total)], None


def slot_spread(slot):
    row = lax.broadcasted_iota(jnp.int32, (LANES, LANES), 0)
    lane = lax.broadcasted_iota(jnp.int32, (LANES, LANES), 1)
    return (row == slot * RANK + lane % RANK).astype(BF16)


def rope_tables(positions):
    half = HD // 2
    frequency = jnp.exp(jnp.arange(half, dtype=F32) * (-2.0 * math.log(ROPE_BASE) / HD))
    angles = positions.astype(F32)[:, None] * frequency[None, :]
    return jnp.cos(angles), jnp.sin(angles)


def head_forward(raw, gain, cosine, sine):
    n = rms(raw, gain)
    half = HD // 2
    a, b = n[:, :half], n[:, half:]
    return jnp.concatenate([a * cosine - b * sine, b * cosine + a * sine], axis=1)


def head_backward(raw, gain, cosine, sine, grad):
    half = HD // 2
    a, b = grad[:, :half], grad[:, half:]
    turned = jnp.concatenate([a * cosine + b * sine, b * cosine - a * sine], axis=1)
    return rms_back(raw, gain, turned)


ROW_BLOCK = 256
VMEM_LIMIT = 67000000
KEY_SPAN = WINDOW + ROW_BLOCK


def rows_at(i, count=ROW_BLOCK):
    return pl.ds(pl.multiple_of(i * count, count), count)


def key_start(i):
    return pl.multiple_of(jnp.maximum(i * ROW_BLOCK - WINDOW, 0), ROW_BLOCK)


def allowed_keys(i, first, segment_column, segment_row):
    rows = i * ROW_BLOCK + lax.broadcasted_iota(jnp.int32, (ROW_BLOCK, KEY_SPAN), 0)
    keys = first + lax.broadcasted_iota(jnp.int32, (ROW_BLOCK, KEY_SPAN), 1)
    gap = rows - keys
    same = segment_column[rows_at(i), :] == segment_row[:, pl.ds(first, KEY_SPAN)]
    return (gap >= 0) & (gap < WINDOW) & same


def weight_copies(sources, target, sems, columns=None):
    out, at = [], 0
    for i, source in enumerate(sources):
        count = source.shape[0]
        part = source if columns is None else source.at[:, columns]
        out.append(pltpu.make_async_copy(part, target.at[pl.ds(at, count)], sems.at[i]))
        at += count
    return out


def with_slots(weight):
    return pltpu.VMEM((weight.shape[0] + LANES, weight.shape[1]), BF16)


def attention_forward_kernel(
    local_heads, scale, normed, enter, leave, gains, cosine, sine, segment_column, segment_row,
    w_qkv, w_o, s_qkv, s_o, raw, qkv, attn, mid_qkv, mid_o, stats, share, w_qkv_here, w_o_here, sems,
):
    copies = [
        weight_copies((w_qkv, s_qkv), w_qkv_here, sems.at[0]),
        weight_copies((w_o, s_o), w_o_here, sems.at[1]),
    ]
    for c in copies[0] + copies[1]:
        c.start()
    blocks = normed.shape[0] // ROW_BLOCK
    key_col = local_heads * HD
    value_col = key_col + HD
    for c in copies[0]:
        c.wait()

    @pl.loop(0, blocks)
    def _(i):
        rows = rows_at(i)
        z = normed[rows, :]
        mid = dot(z, enter[...], BF16)
        mid_qkv[rows, :] = mid
        full = dot(jnp.concatenate([z, mid], axis=1), w_qkv_here[...])
        c, s = cosine[rows, :], sine[rows, :]
        for h in range(local_heads + 1):
            columns = slice(h * HD, (h + 1) * HD)
            gain = gains[0:1, :] if h < local_heads else gains[1:2, :]
            qkv[rows, columns] = head_forward(full[:, columns], gain, c, s).astype(BF16)
        raw[rows, :] = full[:, :value_col]
        qkv[rows, value_col:] = full[:, value_col:].astype(BF16)

    for c in copies[1]:
        c.wait()

    @pl.loop(0, blocks)
    def _(i):
        rows = rows_at(i)
        first = key_start(i)
        keys = qkv[pl.ds(first, KEY_SPAN), key_col:value_col]
        values = qkv[pl.ds(first, KEY_SPAN), value_col:]
        mask = allowed_keys(i, first, segment_column, segment_row)
        for h in range(local_heads):
            scores = dot_nt(qkv[rows, h * HD : (h + 1) * HD], keys) * scale
            scores = jnp.where(mask, scores, NEG_FILL)
            top = jnp.max(scores, axis=-1, keepdims=True)
            expon = jnp.exp(scores - top)
            total = jnp.sum(expon, axis=-1, keepdims=True)
            probs = (expon / total).astype(BF16)
            attn[rows, h * HD : (h + 1) * HD] = dot(probs, values, BF16)
            stats[rows, h * LANES : (h + 1) * LANES] = jnp.broadcast_to(
                top + jnp.log(total), (ROW_BLOCK, LANES)
            )
        both = dot_nt(attn[rows, :], w_o_here[...])
        mid = both[:, -LANES:].astype(BF16)
        mid_o[rows, :] = mid
        share[rows, :] = (both[:, :-LANES] + dot(mid, leave[...])).astype(BF16)


def attention_forward(normed, enter, leave, gains, cosine, sine, segments, qkv_parts, o_parts, scale):
    w_qkv, w_o = qkv_parts[0], o_parts[0]
    length, width = normed.shape
    columns = w_qkv.shape[1]
    local_heads = columns // HD - 2
    shapes = [
        ((length, columns - HD), F32), ((length, columns), BF16), ((length, local_heads * HD), BF16),
        ((length, LANES), BF16), ((length, LANES), BF16), ((length, local_heads * LANES), F32),
        ((length, width), BF16),
    ]
    vmem = pl.BlockSpec(memory_space=pltpu.VMEM)
    return pl.pallas_call(
        functools.partial(attention_forward_kernel, local_heads, scale),
        out_shape=[jax.ShapeDtypeStruct(*shape) for shape in shapes],
        in_specs=[vmem] * 8 + [pl.BlockSpec(memory_space=pl.ANY)] * 4,
        out_specs=[vmem] * len(shapes),
        scratch_shapes=[
            with_slots(w_qkv), with_slots(w_o), pltpu.SemaphoreType.DMA((2, 2)),
        ],
        name="attention_forward",
    )(normed, enter, leave, gains, cosine, sine, segments[:, None], segments[None, :], w_qkv, w_o,
        qkv_parts[1], o_parts[1])


def fold_rows(wide):
    row = lax.broadcasted_iota(jnp.int32, wide.shape, 0)
    lane = lax.broadcasted_iota(jnp.int32, wide.shape, 1)
    kept = jnp.where((lane % LANES) // RANK == row % GROUPS, wide, 0.0)
    return jnp.sum(kept.reshape(wide.shape[0] // GROUPS, GROUPS, wide.shape[1]), axis=1).astype(BF16)


def attention_backward_kernel(
    local_heads, scale, grad_branch, enter, leave, gains, segment_column, segment_row, spread, *refs
):
    distant, refs = refs[:9], refs[9:]
    w_qkv, w_o, s_qkv, s_o, share, entry_qkv, entry_o, exit_qkv, exit_o = refs[:9]
    w_qkv_here, w_o_here, grad_attn, grad_raw, grad_k, grad_v, spread_qkv, spread_o, sems = refs[9:18]
    near, near_sems = refs[18:27], refs[27]
    loads = [pltpu.make_async_copy(*pair, near_sems.at[i]) for i, pair in enumerate(zip(distant, near))]
    qkv, stats, raw, cosine, sine, normed, attn, mid_qkv, mid_o = near
    copies = [
        weight_copies((w_o, s_o), w_o_here, sems.at[0]),
        weight_copies((w_qkv, s_qkv), w_qkv_here, sems.at[1]),
    ]
    for c in copies[0] + loads[:5] + copies[1] + loads[5:]:
        c.start()
    blocks = grad_branch.shape[0] // ROW_BLOCK
    key_col = local_heads * HD
    value_col = key_col + HD
    grad_k[...] = jnp.zeros_like(grad_k)
    grad_v[...] = jnp.zeros_like(grad_v)
    for c in copies[0]:
        c.wait()

    @pl.loop(0, blocks)
    def _(i):
        rows = rows_at(i)
        g = grad_branch[rows, :]
        mid = dot_nt(g, leave[...], BF16)
        spread_o[rows, :] = dot(mid, spread[:, :LANES], BF16)
        grad_attn[rows, :] = dot(jnp.concatenate([g, mid], axis=1), w_o_here[...], BF16)

    for c in loads[:5]:
        c.wait()

    @pl.loop(0, blocks)
    def _(i):
        rows = rows_at(i)
        first = key_start(i)
        span = pl.ds(first, KEY_SPAN)
        keys = qkv[span, key_col:value_col]
        values = qkv[span, value_col:]
        mask = allowed_keys(i, first, segment_column, segment_row)
        for h in range(local_heads):
            columns = slice(h * HD, (h + 1) * HD)
            q = qkv[rows, columns]
            g = grad_attn[rows, columns]
            scores = jnp.where(mask, dot_nt(q, keys) * scale, NEG_FILL)
            probs = jnp.exp(scores - stats[rows, h * LANES : h * LANES + 1])
            grad_probs = dot_nt(g, values)
            inner = jnp.sum(probs * grad_probs, axis=-1, keepdims=True)
            grad_scores = (probs * (grad_probs - inner)).astype(BF16)
            grad_q = dot(grad_scores, keys) * scale
            grad_k[span, :] += dot_tn(grad_scores, q) * scale
            grad_v[span, :] += dot_tn(probs.astype(BF16), g)
            grad_raw[rows, columns] = head_backward(
                raw[rows, columns], gains[0:1, :], cosine[rows, :], sine[rows, :], grad_q
            ).astype(BF16)

    for c in copies[1]:
        c.wait()

    @pl.loop(0, blocks)
    def _(i):
        rows = rows_at(i)
        grad_raw[rows, key_col:value_col] = head_backward(
            raw[rows, key_col:value_col], gains[1:2, :], cosine[rows, :], sine[rows, :], grad_k[rows, :]
        ).astype(BF16)
        grad_raw[rows, value_col:] = grad_v[rows, :].astype(BF16)
        both = dot_nt(grad_raw[rows, :], w_qkv_here[...])
        mid = both[:, -LANES:].astype(BF16)
        spread_qkv[rows, :] = dot(mid, spread[...], BF16)
        share[rows, :] = (both[:, :-LANES] + dot_nt(mid, enter[...])).astype(BF16)

    for c in loads[5:]:
        c.wait()

    @pl.loop(0, normed.shape[1] // LANES)
    def _(j):
        wide = dot_tn(normed[:, rows_at(j, LANES)], spread_qkv[...])
        entry_qkv[rows_at(j, RANK), :] = fold_rows(wide)

    @pl.loop(0, attn.shape[1] // LANES)
    def _(j):
        wide = dot_tn(attn[:, rows_at(j, LANES)], spread_o[...])
        entry_o[rows_at(j, RANK), :] = fold_rows(wide)

    exits = (ADAPTER_SCALING * dot_tn(mid_qkv[...], grad_raw[...])).astype(BF16)
    exit_qkv[:, :key_col] = exits[:RANK, :key_col]
    exit_qkv[:, key_col:value_col] = exits[RANK : 2 * RANK, key_col:value_col]
    exit_qkv[:, value_col:] = exits[2 * RANK : 3 * RANK, value_col:]
    exit_o[...] = (ADAPTER_SCALING * dot_tn(mid_o[...], grad_branch[...]))[:RANK].astype(BF16)


def attention_backward(
    grad_branch, enter, leave, gains, cosine, sine, segments, kept, qkv_parts, o_parts, scale
):
    w_qkv, w_o = qkv_parts[0], o_parts[0]
    length, width = grad_branch.shape
    columns = w_qkv.shape[1]
    local_heads = columns // HD - 2
    spread = jnp.concatenate([slot_spread(i) for i in range(3)], axis=1)
    distant = [
        kept["qkv"], kept["stats"], kept["raw"], cosine, sine, kept["normed"], kept["attn"],
        kept["mid_qkv"], kept["mid_o"],
    ]
    shapes = [
        (length, width), (width // GROUPS, 3 * LANES), (local_heads * HD // GROUPS, LANES),
        (RANK, columns), (RANK, width),
    ]
    vmem = pl.BlockSpec(memory_space=pltpu.VMEM)
    return pl.pallas_call(
        functools.partial(attention_backward_kernel, local_heads, scale),
        out_shape=[jax.ShapeDtypeStruct(shape, BF16) for shape in shapes],
        in_specs=[vmem] * 7 + [pl.BlockSpec(memory_space=pl.ANY)] * 13,
        out_specs=[vmem] * len(shapes),
        scratch_shapes=[
            with_slots(w_qkv), with_slots(w_o),
            pltpu.VMEM((length, local_heads * HD), BF16), pltpu.VMEM((length, columns), BF16),
            pltpu.VMEM((length, HD), F32), pltpu.VMEM((length, HD), F32),
            pltpu.VMEM((length, 3 * LANES), BF16), pltpu.VMEM((length, LANES), BF16),
            pltpu.SemaphoreType.DMA((2, 2)),
        ]
        + [pltpu.VMEM(a.shape, a.dtype) for a in distant]
        + [pltpu.SemaphoreType.DMA((len(distant),))],
        name="attention_backward",
    )(
        grad_branch, enter, leave, gains, segments[:, None], segments[None, :], spread, *distant,
        w_qkv, w_o, qkv_parts[1], o_parts[1],
    )


def gelu_parts(v):
    c = math.sqrt(2.0 / math.pi)
    th = jnp.tanh(c * (v + 0.044715 * v * v * v))
    value = 0.5 * v * (1.0 + th)
    slope = 0.5 * (1.0 + th) + 0.5 * v * (1.0 - th * th) * (c * (1.0 + 3.0 * 0.044715 * v * v))
    return value, slope


FFN_BLOCK = 1280


def ffn_fetch(weights, offsets, buffers, sems, k, j, slot, count):
    source, slots = weights[2 * k], weights[2 * k + 1]
    start = pl.multiple_of(j * FFN_BLOCK, LANES)
    rows = source.shape[0]
    here = buffers.at[k, slot]
    return [
        pltpu.make_async_copy(
            source.at[:, pl.ds(offsets[k] + start, count)],
            here.at[pl.ds(0, rows), pl.ds(0, count)],
            sems.at[k, slot, 0],
        ),
        pltpu.make_async_copy(
            slots.at[:, pl.ds(start, count)],
            here.at[pl.ds(rows, LANES), pl.ds(0, count)],
            sems.at[k, slot, 1],
        ),
    ]


def ffn_start(weights, offsets, buffers, sems, order, columns):
    j = pl.program_id(0)
    steps = pl.cdiv(columns, FFN_BLOCK)

    def start(step, slot, count):
        for k in order:
            for c in ffn_fetch(weights, offsets, buffers, sems, k, step, slot, count):
                c.start()

    @pl.when(j == 0)
    def _():
        start(0, 0, FFN_BLOCK)

    @pl.when(j + 1 < steps - 1)
    def _():
        start(j + 1, 1 - j % 2, FFN_BLOCK)

    @pl.when(j + 1 == steps - 1)
    def _():
        start(j + 1, 1 - j % 2, columns - (steps - 1) * FFN_BLOCK)


def by_width(columns, step):
    steps = pl.cdiv(columns, FFN_BLOCK)
    last = pl.program_id(0) == steps - 1
    pl.when(jnp.logical_not(last))(functools.partial(step, FFN_BLOCK))
    pl.when(last)(functools.partial(step, columns - (steps - 1) * FFN_BLOCK))


def add_to(total, part):
    j = pl.program_id(0)

    @pl.when(j == 0)
    def _():
        total[...] = part

    @pl.when(j > 0)
    def _():
        total[...] += part


def ffn_forward_kernel(
    offsets, columns, z, enter, leave, w_g, s_g, w_u, s_u, w_d, s_d,
    gelu, slope, hidden, mid_gu, mid_d, share, buffers, joined, total, sems,
):
    j = pl.program_id(0)
    slot = j % 2
    width = z.shape[1]
    blocks = z.shape[0] // ROW_BLOCK
    weights = (w_g, s_g, w_u, s_u, w_d, s_d)
    ffn_start(weights, offsets, buffers, sems, (0, 1, 2), columns)

    @pl.when(j == 0)
    def _():
        mid = dot(z[...], enter[...], BF16)
        mid_gu[...] = mid
        joined[:, :width] = z[...]
        joined[:, width:] = mid

    def step(count):
        def wait(k):
            for c in ffn_fetch(weights, offsets, buffers, sems, k, j, slot, count):
                c.wait()

        wait(0)
        wait(1)

        @pl.loop(0, blocks)
        def _(i):
            rows = rows_at(i)
            gate_pre = dot(joined[rows, :], buffers[0, slot, :, :count])
            up_pre = dot(joined[rows, :], buffers[1, slot, :, :count])
            value, rate = gelu_parts(gate_pre)
            gelu[rows, :count] = value.astype(BF16)
            slope[rows, :count] = (rate * up_pre).astype(BF16)
            hidden[rows, :count] = (value * up_pre).astype(BF16)

        wait(2)
        add_to(total, dot_nt(hidden[:, :count], buffers[2, slot, :, :count]))

    by_width(columns, step)

    @pl.when(j == pl.num_programs(0) - 1)
    def _():
        mid = total[:, width:].astype(BF16)
        mid_d[...] = mid
        share[...] = (total[:, :width] + dot(mid, leave[...])).astype(BF16)


def ffn_forward(z, enter, leave, weights, offsets):
    length, width = z.shape
    columns = weights[1].shape[1]
    steps = pl.cdiv(columns, FFN_BLOCK)

    def fixed(shape):
        return pl.BlockSpec(shape, lambda j: (0, 0), pipeline_mode=pl.Buffered(1))

    wide = pl.BlockSpec((length, FFN_BLOCK), lambda j: (0, j))
    hbm = pl.BlockSpec(memory_space=pl.ANY)
    small = (length, LANES)
    return pl.pallas_call(
        functools.partial(ffn_forward_kernel, offsets, columns),
        grid=(steps,),
        out_shape=[jax.ShapeDtypeStruct((length, columns), BF16)] * 3
        + [jax.ShapeDtypeStruct(small, BF16)] * 2
        + [jax.ShapeDtypeStruct((length, width), BF16)],
        in_specs=[fixed(z.shape), fixed(enter.shape), fixed(leave.shape)] + [hbm] * 6,
        out_specs=[wide] * 3 + [fixed(small), fixed(small), fixed((length, width))],
        scratch_shapes=[
            pltpu.VMEM((3, 2, width + LANES, FFN_BLOCK), BF16),
            pltpu.VMEM((length, width + LANES), BF16),
            pltpu.VMEM((length, width + LANES), F32),
            pltpu.SemaphoreType.DMA((3, 2, 2)),
        ],
        compiler_params=pltpu.CompilerParams(vmem_limit_bytes=VMEM_LIMIT),
        name="ffn_forward",
    )(z, enter, leave, *weights)


def ffn_backward_kernel(
    offsets, columns, grad, z, enter, leave, mid_gu, mid_d, spread, gelu, slope, hidden,
    w_g, s_g, w_u, s_u, w_d, s_d,
    share, exit_g, exit_u, entry_d, exit_d, entry_gu,
    buffers, joined, grad_g, grad_u, total, spread_d, spread_gu, sems,
):
    j = pl.program_id(0)
    slot = j % 2
    width = z.shape[1]
    blocks = z.shape[0] // ROW_BLOCK
    weights = (w_g, s_g, w_u, s_u, w_d, s_d)
    ffn_start(weights, offsets, buffers, sems, (2, 0, 1), columns)

    @pl.when(j == 0)
    def _():
        mid = dot_nt(grad[...], leave[...], BF16)
        joined[:, :width] = grad[...]
        joined[:, width:] = mid
        spread_d[...] = dot(mid, spread[:, :LANES], BF16)
        exit_d[...] = (ADAPTER_SCALING * dot_tn(mid_d[...], grad[...]))[:RANK].astype(BF16)

    def step(count):
        def wait(k):
            for c in ffn_fetch(weights, offsets, buffers, sems, k, j, slot, count):
                c.wait()

        wait(2)

        @pl.loop(0, blocks)
        def _(i):
            rows = rows_at(i)
            grad_hidden = dot(joined[rows, :], buffers[2, slot, :, :count])
            grad_g[rows, :count] = (grad_hidden * slope[rows, :count].astype(F32)).astype(BF16)
            grad_u[rows, :count] = (grad_hidden * gelu[rows, :count].astype(F32)).astype(BF16)

        exit_g[:, :count] = (ADAPTER_SCALING * dot_tn(mid_gu[...], grad_g[:, :count]))[:RANK].astype(BF16)
        exit_u[:, :count] = (ADAPTER_SCALING * dot_tn(mid_gu[...], grad_u[:, :count]))[
            RANK : 2 * RANK
        ].astype(BF16)
        wait(0)
        wait(1)
        add_to(
            total,
            dot_nt(grad_g[:, :count], buffers[0, slot, :, :count])
            + dot_nt(grad_u[:, :count], buffers[1, slot, :, :count]),
        )

        @pl.loop(0, count // LANES)
        def _(i):
            wide = dot_tn(hidden[:, rows_at(i, LANES)], spread_d[...])
            entry_d[rows_at(i, RANK), :] = fold_rows(wide)

    by_width(columns, step)

    @pl.when(j == pl.num_programs(0) - 1)
    def _():
        mid = total[:, width:].astype(BF16)
        share[...] = (total[:, :width] + dot_nt(mid, enter[...])).astype(BF16)
        spread_gu[...] = dot(mid, spread[...], BF16)

        @pl.loop(0, width // LANES)
        def _(i):
            wide = dot_tn(z[:, rows_at(i, LANES)], spread_gu[...])
            entry_gu[rows_at(i, RANK), :] = fold_rows(wide)


def ffn_backward(grad, z, enter, leave, kept, weights, offsets):
    length, width = z.shape
    columns = weights[1].shape[1]
    steps = pl.cdiv(columns, FFN_BLOCK)
    spread = jnp.concatenate([slot_spread(i) for i in range(2)], axis=1)

    def fixed(shape):
        return pl.BlockSpec(shape, lambda j: (0, 0), pipeline_mode=pl.Buffered(1))

    wide = pl.BlockSpec((length, FFN_BLOCK), lambda j: (0, j))
    hbm = pl.BlockSpec(memory_space=pl.ANY)
    small = (length, LANES)
    shapes = [
        (length, width), (RANK, columns), (RANK, columns), (columns // GROUPS, LANES), (RANK, width),
        (width // GROUPS, 2 * LANES),
    ]
    narrow = pl.BlockSpec((RANK, FFN_BLOCK), lambda j: (0, j))
    return pl.pallas_call(
        functools.partial(ffn_backward_kernel, offsets, columns),
        grid=(steps,),
        out_shape=[jax.ShapeDtypeStruct(shape, BF16) for shape in shapes],
        in_specs=[
            fixed(grad.shape), fixed(z.shape), fixed(enter.shape), fixed(leave.shape), fixed(small),
            fixed(small), fixed(spread.shape), wide, wide, wide,
        ] + [hbm] * 6,
        out_specs=[
            fixed((length, width)), narrow, narrow,
            pl.BlockSpec((FFN_BLOCK // GROUPS, LANES), lambda j: (j, 0)),
            fixed((RANK, width)), fixed((width // GROUPS, 2 * LANES)),
        ],
        scratch_shapes=[
            pltpu.VMEM((3, 2, width + LANES, FFN_BLOCK), BF16),
            pltpu.VMEM((length, width + LANES), BF16),
            pltpu.VMEM((length, FFN_BLOCK), BF16),
            pltpu.VMEM((length, FFN_BLOCK), BF16),
            pltpu.VMEM((length, width + LANES), F32),
            pltpu.VMEM(small, BF16),
            pltpu.VMEM((length, 2 * LANES), BF16),
            pltpu.SemaphoreType.DMA((3, 2, 2)),
        ],
        compiler_params=pltpu.CompilerParams(vmem_limit_bytes=VMEM_LIMIT),
        name="ffn_backward",
    )(
        grad, z, enter, leave, kept["mid_gu"], kept["mid_d"], spread, kept["gelu"], kept["slope"],
        kept["hidden"], *weights,
    )


def piece_starts(layer_idx):
    starts, at = {}, layer_idx * sum(n for _, n in PIECES) * RANK // LANES
    for name, n in PIECES:
        starts[name] = at
        at += n * RANK // LANES
    return starts


def unpack_kernel(head_cols, hidden_cols, rows, *refs):
    outs, (values, tall) = refs[:-2], refs[-2:]
    tp_place = lax.axis_index("tp")
    sizes = dict(PIECES)

    @pl.loop(0, rows.shape[0] // 16)
    def _(i):
        at = pl.ds(pl.multiple_of(i * 16, 16), 16)
        values[at, :] = rows[at, :].astype(F32)

    def entries(names, starts, count):
        lane = lax.broadcasted_iota(jnp.int32, (count, LANES), 1)
        for s in range(GROUPS):
            row = jnp.zeros((count, LANES), F32)
            for i, start in enumerate(starts):
                moved = values[pl.ds(start, count), :]
                if (i - s) % GROUPS:
                    moved = pltpu.roll(moved, (i - s) % GROUPS * RANK, 1)
                row = jnp.where(lane // RANK == i, moved, row)
            tall[pl.ds(s, count, stride=GROUPS), :] = row

    def exit_rows(out, start, stride, columns, slot, scale):
        for j in range((columns.stop - columns.start) // LANES):
            block = values[pl.ds(start + j, RANK, stride=stride), :] * scale
            at = columns.start + j * LANES
            out[slot * RANK : (slot + 1) * RANK, at : at + LANES] = block.astype(BF16)

    for l in range(LAYERS):
        starts = piece_starts(l)
        enter_qkv, enter_gu, leave_o, leave_d, s_qkv, s_o, s_g, s_u, s_d = outs[9 * l : 9 * l + 9]
        for out in (leave_o, leave_d, s_qkv, s_g, s_u):
            out[...] = jnp.zeros_like(out)
        for out, names in ((enter_qkv, ("Eq", "Ek", "Ev")), (enter_gu, ("Eg", "Eu"))):
            entries(names, [starts[n] for n in names], D // GROUPS)
            out[...] = tall[:D, :].astype(BF16)
        for out, name, columns in ((s_o, "Eo", head_cols), (s_d, "Ed", hidden_cols)):
            count = columns // GROUPS
            entries((name,), [pl.multiple_of(starts[name] + tp_place * count, 8)], count)
            for j in range(columns // LANES):
                at = slice(j * LANES, (j + 1) * LANES)
                out[:, at] = tall[at, :].T.astype(BF16)
        exit_rows(leave_o, starts["Xo"], D // LANES, slice(0, D), 0, ADAPTER_SCALING)
        exit_rows(leave_d, starts["Xd"], D // LANES, slice(0, D), 0, ADAPTER_SCALING)
        for out, name, columns, slot in (
            (s_qkv, "Xq", slice(0, head_cols), 0),
            (s_qkv, "Xk", slice(head_cols, head_cols + HD), 1),
            (s_qkv, "Xv", slice(head_cols + HD, head_cols + 2 * HD), 2),
            (s_g, "Xg", slice(0, hidden_cols), 0),
            (s_u, "Xu", slice(0, hidden_cols), 1),
        ):
            stride = sizes[name] // LANES
            width = (columns.stop - columns.start) // LANES
            first = starts[name] + (tp_place * width if width < stride else 0)
            exit_rows(out, first, stride, columns, slot, ADAPTER_SCALING)


def unpack(own_rows, head_cols, hidden_cols):
    shapes = [
        (D, LANES), (D, LANES), (LANES, D), (LANES, D), (LANES, head_cols + 2 * HD),
        (LANES, head_cols), (LANES, hidden_cols), (LANES, hidden_cols), (LANES, hidden_cols),
    ]
    vmem = pl.BlockSpec(memory_space=pltpu.VMEM)
    got = pl.pallas_call(
        functools.partial(unpack_kernel, head_cols, hidden_cols),
        out_shape=[jax.ShapeDtypeStruct(shape, BF16) for shape in shapes * LAYERS],
        in_specs=[vmem],
        out_specs=[vmem] * (len(shapes) * LAYERS),
        scratch_shapes=[
            pltpu.VMEM(own_rows.shape, F32), pltpu.VMEM((max(D, hidden_cols), LANES), F32),
        ],
        name="unpack",
    )(own_rows)
    maps, spares = [], []
    for l in range(LAYERS):
        part = got[9 * l : 9 * l + 9]
        maps.append(dict(zip(("enter_qkv", "enter_gu", "leave_o", "leave_d"), part)))
        spares.append(dict(zip(("qkv", "o", "g", "u", "d"), part[4:])))
    return maps, spares


def shards(
    hidden_in, out_grad, segments, positions, set_ids, query_w, key_w, value_w, out_w, gate_w,
    up_w, down_w, norm_gains, head_gains, adapters, first_moment, second_moment,
):
    tp_count = lax.axis_size("tp")
    fsdp_count = lax.axis_size("fsdp")
    tp_place = lax.axis_index("tp")
    set_count, share = adapters.shape
    head_cols = HEADS * HD // tp_count
    hidden_cols = FF // tp_count
    scale = HD ** (-0.5)
    set_range = jnp.arange(set_count, dtype=jnp.int32)

    master_low = adapters.astype(BF16)
    selector = (set_ids[:, None] == set_range[None, :]).astype(BF16)
    routed = dot(selector, master_low, BF16)
    whole_rows = share % LANES == 0
    tile = (share // LANES, LANES) if whole_rows else (1, share)
    routed = routed.reshape((fsdp_count,) + tile)
    own = lax.all_to_all(routed, "fsdp", split_axis=0, concat_axis=0, tiled=True)

    def local_weights(l):
        return {
            "qkv": jnp.concatenate([query_w[l], key_w[l], value_w[l]], axis=1),
            "o": out_w[l].T,
            "g": gate_w[l],
            "u": up_w[l],
            "d": down_w[l].T,
        }

    local = [local_weights(l) for l in range(LAYERS)]
    first_names = [(0, "qkv"), (0, "o"), (0, "g"), (0, "u"), (0, "d"), (1, "qkv"), (1, "o"), (1, "g")]
    late = jnp.concatenate([local[1]["u"], local[1]["d"]], axis=1)
    arrays = [local[l][name] for l, name in first_names]
    if fsdp_count == 16:
        part = hidden_cols * 4 // 9 // LANES * LANES
        plan = [
            ("zxy", 0, (0, arrays[0].shape[1])), ("zxy", 1, (0, arrays[1].shape[1])),
            ("zyx", 5, (0, arrays[5].shape[1])), ("zyx", 6, (0, arrays[6].shape[1])),
            ("zxy", 2, (0, hidden_cols)), ("zyx", 3, (0, hidden_cols)),
            ("xyz", 4, (part, hidden_cols - part)), ("yxz", 7, (part, hidden_cols - part)),
            ("zxy", 4, (0, part)), ("zyx", 7, (0, part)),
        ]
        first = gather_weights(arrays, plan, fsdp_count, 11)
    else:
        first = [lax.all_gather(a, "fsdp", axis=0, tiled=True) for a in arrays]
    own, late, first = lax.optimization_barrier((own, late, first))
    late_all = lax.all_gather(late, "fsdp", axis=0, tiled=True)

    own = pair_gather(own, 13)
    own_rows = own.reshape(-1, LANES) if whole_rows else own.reshape(-1).reshape(-1, LANES)
    maps, spares = unpack(own_rows, head_cols, hidden_cols)

    weights = [dict(), dict()]
    for (l, name), array in zip(first_names, first):
        weights[l][name] = (array, spares[l][name])
    weights[1]["u"] = (late_all, spares[1]["u"])
    weights[1]["d"] = (late_all, spares[1]["d"])
    ffn_weights = [w["g"] + w["u"] + w["d"] for w in weights]
    ffn_offsets = [(0, 0, 0), (0, 0, hidden_cols)]
    cosine, sine = rope_tables(positions)
    gains = norm_gains.astype(F32)
    heads = head_gains.astype(F32)

    def gain(l, i):
        return gains[l, i][None, :]

    kept = []
    normed = exchange(body_enter, 1, "enter", None, [hidden_in], [gain(0, 0)], [], True)[0]
    x = hidden_in
    for l in range(LAYERS):
        w = weights[l]
        r = {"x": x, "normed": normed}
        m = maps[l]
        (
            r["raw"], r["qkv"], r["attn"], r["mid_qkv"], r["mid_o"], r["stats"], share_o,
        ) = attention_forward(
            normed, m["enter_qkv"], m["leave_o"], heads[l], cosine, sine, segments, w["qkv"],
            w["o"], scale,
        )
        r["attn_branch"], r["middle"], r["normed_two"] = exchange(
            body_middle, 2 if l == 0 else 3, "middle", share_o, [x], [gain(l, 1), gain(l, 2)],
            [F32, F32], True,
        )
        r["gelu"], r["slope"], r["hidden"], r["mid_gu"], r["mid_d"], share_f = ffn_forward(
            r["normed_two"], m["enter_gu"], m["leave_d"], ffn_weights[l], ffn_offsets[l]
        )
        if l + 1 < LAYERS:
            r["ffn_branch"], x, normed = exchange(
                body_next, 4, "next", share_f, [r["middle"]], [gain(l, 3), gain(l + 1, 0)],
                [F32, F32], True,
            )
        else:
            result, grad_ffn = exchange(
                body_turn, 5, "turn", share_f, [r["middle"], out_grad], [gain(l, 3)], [BF16], True
            )
        kept.append(r)

    grad_out = out_grad
    layer_grads = [None] * LAYERS
    for l in reversed(range(LAYERS)):
        w, r, m = weights[l], kept[l], maps[l]
        pieces = {}

        share_n2, pieces["Xg"], pieces["Xu"], pieces["Ed"], pieces["Xd"], entry_gu = ffn_backward(
            grad_ffn, r["normed_two"], m["enter_gu"], m["leave_d"], r, ffn_weights[l], ffn_offsets[l]
        )
        pieces["Eg"], pieces["Eu"] = entry_gu[:, :LANES], entry_gu[:, LANES:]
        grad_middle, grad_branch = exchange(
            body_back_middle, 6 if l == 1 else 7, "back_middle", share_n2,
            [grad_out, r["middle"], r["attn_branch"]], [gain(l, 2), gain(l, 1)], [F32], True,
        )
        share_n, entry_qkv, pieces["Eo"], exit_qkv, pieces["Xo"] = attention_backward(
            grad_branch, m["enter_qkv"], m["leave_o"], heads[l], cosine, sine, segments, r, w["qkv"],
            w["o"], scale,
        )
        for i, name in enumerate("qkv"):
            pieces["E" + name] = entry_qkv[:, i * LANES : (i + 1) * LANES]
        pieces["Xq"] = exit_qkv[:, :head_cols]
        pieces["Xk"] = exit_qkv[:, head_cols : head_cols + HD]
        pieces["Xv"] = exit_qkv[:, head_cols + HD :]
        if l > 0:
            grad_out, grad_ffn = exchange(
                body_back_next, 8, "back_next", share_n,
                [grad_middle, r["x"], kept[l - 1]["ffn_branch"]], [gain(l, 0), gain(l - 1, 3)],
                [F32], True,
            )
        else:
            grad_out = exchange(
                body_back_last, 9, "back_last", share_n, [grad_middle, r["x"]], [gain(l, 0)], [F32], False
            )[0]
        rows = []
        for name, n in PIECES:
            piece = pieces[name]
            if name in ("Eo", "Ed"):
                piece = lax.dynamic_update_slice_in_dim(
                    jnp.zeros((n * RANK // LANES, LANES), BF16), piece, tp_place * piece.shape[0], 0
                )
            if name in ("Xq", "Xg", "Xu"):
                piece = lax.dynamic_update_slice_in_dim(
                    jnp.zeros((RANK, n), BF16), piece, tp_place * piece.shape[1], 1
                )
            rows.append(piece.reshape(-1, LANES))
        layer_grads[l] = rows

    flat = jnp.concatenate(layer_grads[0] + layer_grads[1], axis=0)
    if whole_rows:
        flat = flat.reshape(fsdp_count * tp_count, share // LANES, LANES)
    else:
        flat = flat.reshape(-1).reshape(fsdp_count * tp_count, 1, share)
    chip_sum = pair_sum(flat, 10)
    arrived = lax.all_to_all(chip_sum, "fsdp", split_axis=0, concat_axis=0, tiled=True).reshape(fsdp_count, share)
    owner_pick = (set_range[:, None] == set_ids[None, :]).astype(BF16)
    set_grads = dot(owner_pick, arrived)
    first_new = BETA_ONE * first_moment + (1.0 - BETA_ONE) * set_grads
    second_new = BETA_TWO * second_moment + (1.0 - BETA_TWO) * set_grads * set_grads
    first_hat = first_new / (1.0 - BETA_ONE**ADAM_STEPS)
    second_hat = second_new / (1.0 - BETA_TWO**ADAM_STEPS)
    new_master = adapters - LEARN_RATE * (
        first_hat / (jnp.sqrt(second_hat) + ADAM_EPS) + DECAY_RATE * adapters
    )
    return (
        result, grad_out, set_grads, new_master, first_new, second_new, new_master.astype(BF16),
    )


def solution(mesh):
    return jax.shard_map(
        shards,
        mesh=mesh,
        in_specs=(
            P(("fsdp", "tp"), None),
            P(("fsdp", "tp"), None),
            P("fsdp"),
            P("fsdp"),
            P(),
            P(None, "fsdp", "tp"),
            P(None, "fsdp", None),
            P(None, "fsdp", None),
            P(None, "tp", "fsdp"),
            P(None, "fsdp", "tp"),
            P(None, "fsdp", "tp"),
            P(None, "tp", "fsdp"),
            P(),
            P(),
            P(None, ("fsdp", "tp")),
            P(None, ("fsdp", "tp")),
            P(None, ("fsdp", "tp")),
        ),
        out_specs=(
            P(("fsdp", "tp"), None),
            P(("fsdp", "tp"), None),
            P(None, ("fsdp", "tp")),
            P(None, ("fsdp", "tp")),
            P(None, ("fsdp", "tp")),
            P(None, ("fsdp", "tp")),
            P(None, ("fsdp", "tp")),
        ),
        check_vma=False,
    )
```

```python
import functools
import math

import jax
import jax.numpy as jnp
from jax import lax
from jax.experimental import pallas as pl
from jax.experimental.pallas import tpu as pltpu
from jax.sharding import PartitionSpec as P

D = 1152
HEADS = 4
HD = 256
FF = 6912
WINDOW = 512
RANK = 16
LAYERS = 2
LANES = 128
GROUPS = LANES // RANK

NORM_EPS = 1e-06
ADAPTER_SCALING = 4.0
ROPE_BASE = 10000.0
LEARN_RATE = 0.01
BETA_ONE = 0.5
BETA_TWO = 0.6
ADAM_STEPS = 4.0
ADAM_EPS = 1e-08
DECAY_RATE = 0.1
NEG_FILL = -1e30
F32 = jnp.float32
BF16 = jnp.bfloat16
MESH = pl.DeviceIdType.MESH
EXCHANGE_CHUNKS = 4

PIECES = (
    ("Eq", D), ("Xq", HEADS * HD), ("Ek", D), ("Xk", HD), ("Ev", D), ("Xv", HD),
    ("Eo", HEADS * HD), ("Xo", D), ("Eg", D), ("Xg", FF), ("Eu", D), ("Xu", FF),
    ("Ed", FF), ("Xd", D),
)


def dot(a, b, out=F32):
    return lax.dot_general(a, b, (((1,), (0,)), ((), ())), preferred_element_type=F32).astype(out)


def dot_nt(a, b, out=F32):
    return lax.dot_general(a, b, (((1,), (1,)), ((), ())), preferred_element_type=F32).astype(out)


def dot_tn(a, b, out=F32):
    return lax.dot_general(a, b, (((0,), (0,)), ((), ())), preferred_element_type=F32).astype(out)


def rms(v, gain):
    return v * lax.rsqrt(jnp.mean(v * v, axis=-1, keepdims=True) + NORM_EPS) * (1.0 + gain)


def rms_back(v, gain, dy):
    r = lax.rsqrt(jnp.mean(v * v, axis=-1, keepdims=True) + NORM_EPS)
    scaled = (1.0 + gain) * dy
    return r * scaled - v * (r * r * r) * jnp.mean(v * scaled, axis=-1, keepdims=True)


def exchange_kernel(body, has_partial, n_rows, n_gains, n_outs, has_send, n_chunks, *refs):
    refs = list(refs)

    def take(count):
        out = refs[:count]
        del refs[:count]
        return out

    partial = take(1)[0] if has_partial else None
    rows, gains, outs = take(n_rows), take(n_gains), take(n_outs)
    gathered = take(1)[0] if has_send else None
    rows_here, outs_here = take(n_rows), take(n_outs)
    row_sems, out_sems = take(2)
    if has_partial:
        mine, arrived, mine_sems, send_a, recv_a = take(5)
    if has_send:
        spread_here, keep_sems, send_b, recv_b = take(4)
    me = lax.axis_index("tp")
    other = 1 - me
    half = (partial if has_partial else gathered).shape[0] // 2
    chunk = half // n_chunks

    def span(base, c):
        return pl.ds(pl.multiple_of(base * half + c * chunk, chunk), chunk)

    def local(c):
        return pl.ds(c * chunk, chunk)

    loads = []
    for c in range(n_chunks):
        group = [
            pltpu.make_async_copy(r.at[local(c)], h.at[local(c)], row_sems.at[i, c])
            for i, (r, h) in enumerate(zip(rows, rows_here))
        ]
        if has_partial:
            group.append(
                pltpu.make_async_copy(partial.at[span(me, c)], mine.at[local(c)], mine_sems.at[c])
            )
        for copy in group:
            copy.start()
        loads.append(group)
    barrier = pltpu.get_barrier_semaphore()
    pl.semaphore_signal(barrier, inc=1, device_id={"tp": other}, device_id_type=MESH)
    pl.semaphore_wait(barrier, 1)
    sends, spreads, stores = [], [], []
    if has_partial:
        for c in range(n_chunks):
            copy = pltpu.make_async_remote_copy(
                src_ref=partial.at[span(other, c)],
                dst_ref=arrived.at[local(c)],
                send_sem=send_a.at[c],
                recv_sem=recv_a.at[c],
                device_id={"tp": other},
                device_id_type=MESH,
            )
            copy.start()
            sends.append(copy)
    gain_values = [g[...].astype(F32) for g in gains]

    def release(c):
        if has_send:
            spreads[c].start()
        for copy in stores[c]:
            copy.start()

    for c in range(n_chunks):
        for copy in loads[c]:
            copy.wait()
        total = None
        if has_partial:
            sends[c].wait_recv()
            total = mine[local(c), :].astype(F32) + arrived[local(c), :].astype(F32)
        values, spread = body(total, [r[local(c), :].astype(F32) for r in rows_here], gain_values)
        group = []
        for i, (ref, here, value) in enumerate(zip(outs, outs_here, values)):
            here[local(c), :] = value.astype(here.dtype)
            group.append(pltpu.make_async_copy(here.at[local(c)], ref.at[local(c)], out_sems.at[i, c]))
        if has_send:
            spread_here[local(c), :] = spread.astype(BF16)
            group.append(
                pltpu.make_async_copy(spread_here.at[local(c)], gathered.at[span(me, c)], keep_sems.at[c])
            )
            spreads.append(
                pltpu.make_async_remote_copy(
                    src_ref=spread_here.at[local(c)],
                    dst_ref=gathered.at[span(me, c)],
                    send_sem=send_b.at[c],
                    recv_sem=recv_b.at[c],
                    device_id={"tp": other},
                    device_id_type=MESH,
                )
            )
        stores.append(group)
        if c > 0:
            release(c - 1)
    release(n_chunks - 1)
    for copy in sends:
        copy.wait_send()
    for c in range(n_chunks):
        for copy in stores[c]:
            copy.wait()
    for copy in spreads:
        copy.wait()


def exchange(body, collective_id, name, partial, rows, gains, out_types, has_send, n_chunks=EXCHANGE_CHUNKS):
    operands = ([] if partial is None else [partial]) + list(rows)
    width = operands[0].shape[1]
    half = partial.shape[0] // 2 if partial is not None else rows[0].shape[0]
    outs = [jax.ShapeDtypeStruct((half, width), kind) for kind in out_types]
    scratch = [pltpu.VMEM((half, width), r.dtype) for r in rows]
    scratch += [pltpu.VMEM((half, width), kind) for kind in out_types]
    scratch += [
        pltpu.SemaphoreType.DMA((len(rows), n_chunks)),
        pltpu.SemaphoreType.DMA((max(len(outs), 1), n_chunks)),
    ]
    each = pltpu.SemaphoreType.DMA((n_chunks,))
    if partial is not None:
        scratch += [pltpu.VMEM((half, width), partial.dtype)] * 2 + [each] * 3
    if has_send:
        outs.append(jax.ShapeDtypeStruct((2 * half, width), BF16))
        scratch += [pltpu.VMEM((half, width), BF16)] + [each] * 3
    hbm = pl.BlockSpec(memory_space=pl.ANY)
    return pl.pallas_call(
        functools.partial(
            exchange_kernel, body, partial is not None, len(rows), len(gains), len(out_types),
            has_send, n_chunks,
        ),
        out_shape=outs,
        in_specs=[hbm] * len(operands) + [pl.BlockSpec(memory_space=pltpu.VMEM)] * len(gains),
        out_specs=[hbm] * len(outs),
        scratch_shapes=scratch,
        compiler_params=pltpu.CompilerParams(collective_id=collective_id, has_side_effects=True),
        name=name,
    )(*operands, *gains)


def gather_kernel(plan, nz, rows, n_arrays, *refs):
    mine, gathered = refs[:n_arrays], refs[n_arrays : 2 * n_arrays]
    send_sem, recv_sem, local_sem = refs[2 * n_arrays :]
    f = lax.axis_index("fsdp")
    x, y, z = f % 2, (f // 2) % 2, f // 4

    def index(a, b, c):
        return (a * 2 + b) * 2 + c

    peers = {
        "x": (index(z, y, 1 - x), None),
        "y": (index(z, 1 - y, x), None),
        "u": (f + 4, z < nz - 1),
        "d": (f - 4, z > 0),
    }
    ways_index = "xyud".index

    def guarded(cond, fn):
        if cond is None:
            fn()
        else:
            pl.when(cond)(fn)

    barrier = pltpu.get_barrier_semaphore()

    def greet(peer):
        pl.semaphore_signal(barrier, inc=1, device_id={"fsdp": peer}, device_id_type=MESH)

    for peer, cond in peers.values():
        guarded(cond, functools.partial(greet, peer))
    inside = jnp.logical_and(z > 0, z < nz - 1)
    pl.when(inside)(lambda: pl.semaphore_wait(barrier, 4))
    pl.when(jnp.logical_not(inside))(lambda: pl.semaphore_wait(barrier, 3))

    offsets = [(dz, fy, fx) for dz in range(1 - nz, nz) for fy in (0, 1) for fx in (0, 1)]
    offsets.sort(key=lambda o: (abs(o[0]) + o[1] + o[2], o))
    ids = {o: i for i, o in enumerate(offsets)}
    own = (0, 0, 0)

    def place(array, source, columns):
        return gathered[array].at[pl.ds(pl.multiple_of(source * rows, 8), rows), pl.ds(*columns)]

    for a in range(n_arrays):
        pltpu.make_async_copy(
            mine[a], place(a, f, (0, mine[a].shape[1])), local_sem.at[a]
        ).start()

    def source_of(o):
        return index(z + o[0], y + o[1] - 2 * y * o[1], x + o[2] - 2 * x * o[2])

    def copy(k, o, way):
        target = {
            "u": (o[0] - 1, o[1], o[2]), "d": (o[0] + 1, o[1], o[2]),
            "x": (o[0], o[1], 1), "y": (o[0], 1, o[2]),
        }[way]
        _, array, columns = plan[k]
        block = place(array, source_of(o), columns)
        return pltpu.make_async_remote_copy(
            src_ref=mine[array].at[:, pl.ds(*columns)] if o == own else block,
            dst_ref=block,
            send_sem=send_sem.at[k, ids[o], ways_index(way)],
            recv_sem=recv_sem.at[k, ids[target]],
            device_id={"fsdp": peers[way][0]},
            device_id_type=MESH,
        )

    def arrival(k, o):
        _, array, columns = plan[k]
        block = place(array, source_of(o), columns)
        return pltpu.make_async_remote_copy(
            src_ref=block, dst_ref=block, send_sem=send_sem.at[k, ids[o], 0],
            recv_sem=recv_sem.at[k, ids[o]], device_id={"fsdp": peers["x"][0]}, device_id_type=MESH,
        )

    def ways(order, o):
        used = {"z": o[0] != 0, "y": o[1] != 0, "x": o[2] != 0}
        last = max([i for i, a in enumerate(order) if used[a]], default=-1)
        out = []
        if last >= 0 and order[last] == "z" and abs(o[0]) < nz - 1:
            out.append("d" if o[0] > 0 else "u")
        for a in order[last + 1 :]:
            out += ["u", "d"] if a == "z" else [a]
        return out

    def exists(o):
        if o[0] == 0:
            return None
        return z < nz - o[0] if o[0] > 0 else z >= -o[0]

    def pass_on(k, o):
        if o != own:
            arrival(k, o).wait_recv()
        for way in ways(plan[k][0], o):
            guarded(peers[way][1], lambda way=way: copy(k, o, way).start())

    def finish(k, o):
        for way in ways(plan[k][0], o):
            guarded(peers[way][1], lambda way=way: copy(k, o, way).wait_send())

    for step in (pass_on, finish):
        for o in offsets:
            for k in range(len(plan)):
                guarded(exists(o), functools.partial(step, k, o))
    for a in range(n_arrays):
        pltpu.make_async_copy(
            mine[a], place(a, f, (0, mine[a].shape[1])), local_sem.at[a]
        ).wait()


def gather_weights(arrays, plan, count, collective_id):
    rows = arrays[0].shape[0]
    nz = count // 4
    offsets = (2 * nz - 1) * 4
    return pl.pallas_call(
        functools.partial(gather_kernel, plan, nz, rows, len(arrays)),
        out_shape=[
            jax.ShapeDtypeStruct((count * rows, a.shape[1]), a.dtype) for a in arrays
        ],
        in_specs=[pl.BlockSpec(memory_space=pltpu.VMEM)] * len(arrays),
        out_specs=[pl.BlockSpec(memory_space=pl.ANY)] * len(arrays),
        scratch_shapes=[
            pltpu.SemaphoreType.DMA((len(plan), offsets, 4)),
            pltpu.SemaphoreType.DMA((len(plan), offsets)),
            pltpu.SemaphoreType.DMA((len(arrays),)),
        ],
        compiler_params=pltpu.CompilerParams(collective_id=collective_id, has_side_effects=True),
        name="gather_weights",
    )(*arrays)


def pair_sum_kernel(count, partial, total, arrived, send_sem, recv_sem):
    me = lax.axis_index("tp")
    other = 1 - me
    barrier = pltpu.get_barrier_semaphore()
    pl.semaphore_signal(barrier, inc=1, device_id={"tp": other}, device_id_type=MESH)
    pl.semaphore_wait(barrier, 1)
    copies = []
    for i in range(count):
        copy = pltpu.make_async_remote_copy(
            src_ref=partial.at[2 * i + other], dst_ref=arrived.at[i], send_sem=send_sem.at[i],
            recv_sem=recv_sem.at[i], device_id={"tp": other}, device_id_type=MESH,
        )
        copy.start()
        copies.append(copy)
    for i in range(count):
        copies[i].wait_recv()
        total[i] = (partial[2 * i + me].astype(F32) + arrived[i].astype(F32)).astype(total.dtype)
    for copy in copies:
        copy.wait_send()


def pair_sum(partial, collective_id):
    count = partial.shape[0] // 2
    shape = (count,) + partial.shape[1:]
    vmem = pl.BlockSpec(memory_space=pltpu.VMEM)
    return pl.pallas_call(
        functools.partial(pair_sum_kernel, count),
        out_shape=jax.ShapeDtypeStruct(shape, partial.dtype),
        in_specs=[vmem],
        out_specs=vmem,
        scratch_shapes=[
            pltpu.VMEM(shape, partial.dtype),
            pltpu.SemaphoreType.DMA((count,)),
            pltpu.SemaphoreType.DMA((count,)),
        ],
        compiler_params=pltpu.CompilerParams(collective_id=collective_id, has_side_effects=True),
        name="pair_sum",
    )(partial)


def pair_gather_kernel(count, n_arrays, mine, *refs):
    arrays, both, halves = refs[:n_arrays], refs[n_arrays], refs[n_arrays + 1 : 2 * n_arrays + 1]
    send_sem, recv_sem, local_sem, send_half, recv_half = refs[2 * n_arrays + 1 :]
    me = lax.axis_index("tp")
    other = 1 - me
    barrier = pltpu.get_barrier_semaphore()
    pl.semaphore_signal(barrier, inc=1, device_id={"tp": other}, device_id_type=MESH)
    pl.semaphore_wait(barrier, 1)
    copies = []
    for i in range(count):
        place = both.at[2 * i + me]
        copies.append(
            pltpu.make_async_remote_copy(
                src_ref=mine.at[i], dst_ref=place, send_sem=send_sem.at[i], recv_sem=recv_sem.at[i],
                device_id={"tp": other}, device_id_type=MESH,
            )
        )
        copies.append(pltpu.make_async_copy(mine.at[i], place, local_sem.at[i]))
    for i in range(n_arrays):
        columns = halves[i].shape[1]
        first = arrays[i].shape[1] - columns
        copies.append(
            pltpu.make_async_remote_copy(
                src_ref=arrays[i].at[:, pl.ds(first, columns)], dst_ref=halves[i],
                send_sem=send_half.at[i], recv_sem=recv_half.at[i],
                device_id={"tp": other}, device_id_type=MESH,
            )
        )
    for copy in copies:
        copy.start()
    for copy in copies:
        copy.wait()


def pair_gather(mine, arrays, columns, collective_id):
    count = mine.shape[0]
    hbm = pl.BlockSpec(memory_space=pl.ANY)
    got = pl.pallas_call(
        functools.partial(pair_gather_kernel, count, len(arrays)),
        out_shape=[jax.ShapeDtypeStruct((2 * count,) + mine.shape[1:], mine.dtype)]
        + [jax.ShapeDtypeStruct((a.shape[0], columns), a.dtype) for a in arrays],
        in_specs=[pl.BlockSpec(memory_space=pltpu.VMEM)] + [hbm] * len(arrays),
        out_specs=[hbm] * (1 + len(arrays)),
        scratch_shapes=[pltpu.SemaphoreType.DMA((count,))] * 3
        + [pltpu.SemaphoreType.DMA((len(arrays),))] * 2,
        compiler_params=pltpu.CompilerParams(collective_id=collective_id, has_side_effects=True),
        name="pair_gather",
    )(mine, *arrays)
    return got[0], got[1:]


def body_enter(total, rows, gains):
    return [], rms(rows[0], gains[0])


def body_middle(total, rows, gains):
    middle = rows[0] + rms(total, gains[0])
    return [total, middle], rms(middle, gains[1])


def body_next(total, rows, gains):
    leaving = rows[0] + rms(total, gains[0])
    return [total, leaving], rms(leaving, gains[1])


def body_turn(total, rows, gains):
    leaving = rows[0] + rms(total, gains[0])
    return [leaving], rms_back(total, gains[0], rows[1])


def body_back_middle(total, rows, gains):
    grad_middle = rows[0] + rms_back(rows[1], gains[0], total)
    return [grad_middle], rms_back(rows[2], gains[1], grad_middle)


def body_back_next(total, rows, gains):
    grad_x = rows[0] + rms_back(rows[1], gains[0], total)
    return [grad_x], rms_back(rows[2], gains[1], grad_x)


def body_back_last(total, rows, gains):
    return [rows[0] + rms_back(rows[1], gains[0], total)], None


def slot_spread(slot):
    row = lax.broadcasted_iota(jnp.int32, (LANES, LANES), 0)
    lane = lax.broadcasted_iota(jnp.int32, (LANES, LANES), 1)
    return (row == slot * RANK + lane % RANK).astype(BF16)


def rope_tables(positions):
    half = HD // 2
    frequency = jnp.exp(jnp.arange(half, dtype=F32) * (-2.0 * math.log(ROPE_BASE) / HD))
    angles = positions.astype(F32)[:, None] * frequency[None, :]
    return jnp.cos(angles), jnp.sin(angles)


def head_forward(raw, gain, cosine, sine):
    n = rms(raw, gain)
    half = HD // 2
    a, b = n[:, :half], n[:, half:]
    return jnp.concatenate([a * cosine - b * sine, b * cosine + a * sine], axis=1)


def head_backward(raw, gain, cosine, sine, grad):
    half = HD // 2
    a, b = grad[:, :half], grad[:, half:]
    turned = jnp.concatenate([a * cosine + b * sine, b * cosine - a * sine], axis=1)
    return rms_back(raw, gain, turned)


ROW_BLOCK = 256
VMEM_LIMIT = 67000000
KEY_SPAN = WINDOW + ROW_BLOCK


def rows_at(i, count=ROW_BLOCK):
    return pl.ds(pl.multiple_of(i * count, count), count)


def key_start(i):
    return pl.multiple_of(jnp.maximum(i * ROW_BLOCK - WINDOW, 0), ROW_BLOCK)


def allowed_keys(i, first, segment_column, segment_row):
    rows = i * ROW_BLOCK + lax.broadcasted_iota(jnp.int32, (ROW_BLOCK, KEY_SPAN), 0)
    keys = first + lax.broadcasted_iota(jnp.int32, (ROW_BLOCK, KEY_SPAN), 1)
    gap = rows - keys
    same = segment_column[rows_at(i), :] == segment_row[:, pl.ds(first, KEY_SPAN)]
    return (gap >= 0) & (gap < WINDOW) & same


def weight_copies(sources, target, sems, columns=None):
    out, at = [], 0
    for i, source in enumerate(sources):
        count = source.shape[0]
        part = source if columns is None else source.at[:, columns]
        out.append(pltpu.make_async_copy(part, target.at[pl.ds(at, count)], sems.at[i]))
        at += count
    return out


def qkv_copies(own, slots, partner, target, sems):
    me = lax.axis_index("tp")
    rows, half = own.shape[0], partner.shape[1] // 2
    heads = own.shape[1] - 2 * half
    top = pl.ds(0, rows)

    def columns(part, core):
        return pl.ds(pl.multiple_of(heads + part * 2 * half + core * half, half), half)

    pairs = [
        (own.at[:, pl.ds(0, heads)], target.at[top, pl.ds(0, heads)]),
        (slots, target.at[pl.ds(rows, slots.shape[0])]),
    ]
    for part in range(2):
        pairs.append((own.at[:, pl.ds(heads + part * half, half)], target.at[top, columns(part, me)]))
        pairs.append((partner.at[:, pl.ds(part * half, half)], target.at[top, columns(part, 1 - me)]))
    return [pltpu.make_async_copy(*pair, sems.at[i]) for i, pair in enumerate(pairs)]


def with_slots(parts):
    return pltpu.VMEM((parts[0].shape[0] + LANES, parts[1].shape[1]), BF16)


def attention_forward_kernel(
    local_heads, scale, normed, enter, leave, gains, cosine, sine, segment_column, segment_row,
    w_qkv, w_o, s_qkv, s_o, w_kv, raw, qkv, attn, mid_qkv, mid_o, stats, share, w_qkv_here, w_o_here, sems,
):
    copies = [
        qkv_copies(w_qkv, s_qkv, w_kv, w_qkv_here, sems.at[0]),
        weight_copies((w_o, s_o), w_o_here, sems.at[1]),
    ]
    for c in copies[0] + copies[1]:
        c.start()
    blocks = normed.shape[0] // ROW_BLOCK
    key_col = local_heads * HD
    value_col = key_col + HD
    for c in copies[0]:
        c.wait()

    @pl.loop(0, blocks)
    def _(i):
        rows = rows_at(i)
        z = normed[rows, :]
        mid = dot(z, enter[...], BF16)
        mid_qkv[rows, :] = mid
        full = dot(jnp.concatenate([z, mid], axis=1), w_qkv_here[...])
        c, s = cosine[rows, :], sine[rows, :]
        for h in range(local_heads + 1):
            columns = slice(h * HD, (h + 1) * HD)
            gain = gains[0:1, :] if h < local_heads else gains[1:2, :]
            qkv[rows, columns] = head_forward(full[:, columns], gain, c, s).astype(BF16)
        raw[rows, :] = full[:, :value_col]
        qkv[rows, value_col:] = full[:, value_col:].astype(BF16)

    for c in copies[1]:
        c.wait()

    @pl.loop(0, blocks)
    def _(i):
        rows = rows_at(i)
        first = key_start(i)
        keys = qkv[pl.ds(first, KEY_SPAN), key_col:value_col]
        values = qkv[pl.ds(first, KEY_SPAN), value_col:]
        mask = allowed_keys(i, first, segment_column, segment_row)
        for h in range(local_heads):
            scores = dot_nt(qkv[rows, h * HD : (h + 1) * HD], keys) * scale
            scores = jnp.where(mask, scores, NEG_FILL)
            top = jnp.max(scores, axis=-1, keepdims=True)
            expon = jnp.exp(scores - top)
            total = jnp.sum(expon, axis=-1, keepdims=True)
            probs = (expon / total).astype(BF16)
            attn[rows, h * HD : (h + 1) * HD] = dot(probs, values, BF16)
            stats[rows, h * LANES : (h + 1) * LANES] = jnp.broadcast_to(
                top + jnp.log(total), (ROW_BLOCK, LANES)
            )
        both = dot_nt(attn[rows, :], w_o_here[...])
        mid = both[:, -LANES:].astype(BF16)
        mid_o[rows, :] = mid
        share[rows, :] = (both[:, :-LANES] + dot(mid, leave[...])).astype(BF16)


def attention_forward(normed, enter, leave, gains, cosine, sine, segments, qkv_parts, o_parts, scale):
    w_qkv, w_o = qkv_parts[0], o_parts[0]
    length, width = normed.shape
    columns = qkv_parts[1].shape[1]
    local_heads = columns // HD - 2
    shapes = [
        ((length, columns - HD), F32), ((length, columns), BF16), ((length, local_heads * HD), BF16),
        ((length, LANES), BF16), ((length, LANES), BF16), ((length, local_heads * LANES), F32),
        ((length, width), BF16),
    ]
    vmem = pl.BlockSpec(memory_space=pltpu.VMEM)
    return pl.pallas_call(
        functools.partial(attention_forward_kernel, local_heads, scale),
        out_shape=[jax.ShapeDtypeStruct(*shape) for shape in shapes],
        in_specs=[vmem] * 8 + [pl.BlockSpec(memory_space=pl.ANY)] * 5,
        out_specs=[vmem] * len(shapes),
        scratch_shapes=[
            with_slots(qkv_parts), with_slots(o_parts), pltpu.SemaphoreType.DMA((2, 6)),
        ],
        name="attention_forward",
    )(normed, enter, leave, gains, cosine, sine, segments[:, None], segments[None, :], w_qkv, w_o,
        qkv_parts[1], o_parts[1], qkv_parts[2])


def fold_rows(wide):
    row = lax.broadcasted_iota(jnp.int32, wide.shape, 0)
    lane = lax.broadcasted_iota(jnp.int32, wide.shape, 1)
    kept = jnp.where((lane % LANES) // RANK == row % GROUPS, wide, 0.0)
    return jnp.sum(kept.reshape(wide.shape[0] // GROUPS, GROUPS, wide.shape[1]), axis=1).astype(BF16)


def attention_backward_kernel(
    local_heads, scale, grad_branch, enter, leave, gains, segment_column, segment_row, spread, *refs
):
    distant, refs = refs[:9], refs[9:]
    w_qkv, w_o, s_qkv, s_o, w_kv, share, entry_qkv, entry_o, exit_qkv, exit_o = refs[:10]
    w_qkv_here, w_o_here, grad_attn, grad_raw, grad_k, grad_v, spread_qkv, spread_o, sems = refs[10:19]
    near, near_sems = refs[19:28], refs[28]
    loads = [pltpu.make_async_copy(*pair, near_sems.at[i]) for i, pair in enumerate(zip(distant, near))]
    qkv, stats, raw, cosine, sine, normed, attn, mid_qkv, mid_o = near
    copies = [
        weight_copies((w_o, s_o), w_o_here, sems.at[0]),
        qkv_copies(w_qkv, s_qkv, w_kv, w_qkv_here, sems.at[1]),
    ]
    for c in copies[0] + loads[:5] + copies[1] + loads[5:]:
        c.start()
    blocks = grad_branch.shape[0] // ROW_BLOCK
    key_col = local_heads * HD
    value_col = key_col + HD
    grad_k[...] = jnp.zeros_like(grad_k)
    grad_v[...] = jnp.zeros_like(grad_v)
    for c in copies[0]:
        c.wait()

    @pl.loop(0, blocks, unroll=2)
    def _(i):
        rows = rows_at(i)
        g = grad_branch[rows, :]
        mid = dot_nt(g, leave[...], BF16)
        spread_o[rows, :] = dot(mid, spread[:, :LANES], BF16)
        grad_attn[rows, :] = dot(jnp.concatenate([g, mid], axis=1), w_o_here[...], BF16)

    for c in loads[:5]:
        c.wait()

    @pl.loop(0, blocks, unroll=2)
    def _(i):
        rows = rows_at(i)
        first = key_start(i)
        span = pl.ds(first, KEY_SPAN)
        keys = qkv[span, key_col:value_col]
        values = qkv[span, value_col:]
        mask = allowed_keys(i, first, segment_column, segment_row)
        for h in range(local_heads):
            columns = slice(h * HD, (h + 1) * HD)
            q = qkv[rows, columns]
            g = grad_attn[rows, columns]
            scores = jnp.where(mask, dot_nt(q, keys) * scale, NEG_FILL)
            probs = jnp.exp(scores - stats[rows, h * LANES : h * LANES + 1])
            grad_probs = dot_nt(g, values)
            inner = jnp.sum(probs * grad_probs, axis=-1, keepdims=True)
            grad_scores = (probs * (grad_probs - inner)).astype(BF16)
            grad_q = dot(grad_scores, keys) * scale
            grad_k[span, :] += dot_tn(grad_scores, q) * scale
            grad_v[span, :] += dot_tn(probs.astype(BF16), g)
            grad_raw[rows, columns] = head_backward(
                raw[rows, columns], gains[0:1, :], cosine[rows, :], sine[rows, :], grad_q
            ).astype(BF16)

    for c in copies[1]:
        c.wait()

    @pl.loop(0, blocks, unroll=2)
    def _(i):
        rows = rows_at(i)
        grad_raw[rows, key_col:value_col] = head_backward(
            raw[rows, key_col:value_col], gains[1:2, :], cosine[rows, :], sine[rows, :], grad_k[rows, :]
        ).astype(BF16)
        grad_raw[rows, value_col:] = grad_v[rows, :].astype(BF16)
        both = dot_nt(grad_raw[rows, :], w_qkv_here[...])
        mid = both[:, -LANES:].astype(BF16)
        spread_qkv[rows, :] = dot(mid, spread[...], BF16)
        share[rows, :] = (both[:, :-LANES] + dot_nt(mid, enter[...])).astype(BF16)

    for c in loads[5:]:
        c.wait()

    @pl.loop(0, normed.shape[1] // LANES)
    def _(j):
        wide = dot_tn(normed[:, rows_at(j, LANES)], spread_qkv[...])
        entry_qkv[rows_at(j, RANK), :] = fold_rows(wide)

    @pl.loop(0, attn.shape[1] // LANES)
    def _(j):
        wide = dot_tn(attn[:, rows_at(j, LANES)], spread_o[...])
        entry_o[rows_at(j, RANK), :] = fold_rows(wide)

    exits = (ADAPTER_SCALING * dot_tn(mid_qkv[...], grad_raw[...])).astype(BF16)
    exit_qkv[:, :key_col] = exits[:RANK, :key_col]
    exit_qkv[:, key_col:value_col] = exits[RANK : 2 * RANK, key_col:value_col]
    exit_qkv[:, value_col:] = exits[2 * RANK : 3 * RANK, value_col:]
    exit_o[...] = (ADAPTER_SCALING * dot_tn(mid_o[...], grad_branch[...]))[:RANK].astype(BF16)


def attention_backward(
    grad_branch, enter, leave, gains, cosine, sine, segments, kept, qkv_parts, o_parts, scale
):
    w_qkv, w_o = qkv_parts[0], o_parts[0]
    length, width = grad_branch.shape
    columns = qkv_parts[1].shape[1]
    local_heads = columns // HD - 2
    spread = jnp.concatenate([slot_spread(i) for i in range(3)], axis=1)
    distant = [
        kept["qkv"], kept["stats"], kept["raw"], cosine, sine, kept["normed"], kept["attn"],
        kept["mid_qkv"], kept["mid_o"],
    ]
    shapes = [
        (length, width), (width // GROUPS, 3 * LANES), (local_heads * HD // GROUPS, LANES),
        (RANK, columns), (RANK, width),
    ]
    vmem = pl.BlockSpec(memory_space=pltpu.VMEM)
    return pl.pallas_call(
        functools.partial(attention_backward_kernel, local_heads, scale),
        out_shape=[jax.ShapeDtypeStruct(shape, BF16) for shape in shapes],
        in_specs=[vmem] * 7 + [pl.BlockSpec(memory_space=pl.ANY)] * 14,
        out_specs=[vmem] * len(shapes),
        scratch_shapes=[
            with_slots(qkv_parts), with_slots(o_parts),
            pltpu.VMEM((length, local_heads * HD), BF16), pltpu.VMEM((length, columns), BF16),
            pltpu.VMEM((length, HD), F32), pltpu.VMEM((length, HD), F32),
            pltpu.VMEM((length, 3 * LANES), BF16), pltpu.VMEM((length, LANES), BF16),
            pltpu.SemaphoreType.DMA((2, 6)),
        ]
        + [pltpu.VMEM(a.shape, a.dtype) for a in distant]
        + [pltpu.SemaphoreType.DMA((len(distant),))],
        name="attention_backward",
    )(
        grad_branch, enter, leave, gains, segments[:, None], segments[None, :], spread, *distant,
        w_qkv, w_o, qkv_parts[1], o_parts[1], qkv_parts[2],
    )


def gelu_parts(v):
    c = math.sqrt(2.0 / math.pi)
    th = jnp.tanh(c * (v + 0.044715 * v * v * v))
    value = 0.5 * v * (1.0 + th)
    slope = 0.5 * (1.0 + th) + 0.5 * v * (1.0 - th * th) * (c * (1.0 + 3.0 * 0.044715 * v * v))
    return value, slope


FFN_BLOCK = 1280


def ffn_fetch(weights, offsets, buffers, sems, k, j, slot, count):
    source, slots = weights[2 * k], weights[2 * k + 1]
    start = pl.multiple_of(j * FFN_BLOCK, LANES)
    rows = source.shape[0]
    here = buffers.at[k, slot]
    return [
        pltpu.make_async_copy(
            source.at[:, pl.ds(offsets[k] + start, count)],
            here.at[pl.ds(0, rows), pl.ds(0, count)],
            sems.at[k, slot, 0],
        ),
        pltpu.make_async_copy(
            slots.at[:, pl.ds(start, count)],
            here.at[pl.ds(rows, LANES), pl.ds(0, count)],
            sems.at[k, slot, 1],
        ),
    ]


def ffn_start(weights, offsets, buffers, sems, order, columns):
    j = pl.program_id(0)
    steps = pl.cdiv(columns, FFN_BLOCK)

    def start(step, slot, count):
        for k in order:
            for c in ffn_fetch(weights, offsets, buffers, sems, k, step, slot, count):
                c.start()

    @pl.when(j == 0)
    def _():
        start(0, 0, FFN_BLOCK)

    @pl.when(j + 1 < steps - 1)
    def _():
        start(j + 1, 1 - j % 2, FFN_BLOCK)

    @pl.when(j + 1 == steps - 1)
    def _():
        start(j + 1, 1 - j % 2, columns - (steps - 1) * FFN_BLOCK)


def by_width(columns, step):
    steps = pl.cdiv(columns, FFN_BLOCK)
    last = pl.program_id(0) == steps - 1
    pl.when(jnp.logical_not(last))(functools.partial(step, FFN_BLOCK))
    pl.when(last)(functools.partial(step, columns - (steps - 1) * FFN_BLOCK))


def add_to(total, part):
    j = pl.program_id(0)

    @pl.when(j == 0)
    def _():
        total[...] = part

    @pl.when(j > 0)
    def _():
        total[...] += part


def ffn_forward_kernel(
    offsets, columns, z, enter, leave, w_g, s_g, w_u, s_u, w_d, s_d,
    gelu, slope, hidden, mid_gu, mid_d, share, buffers, joined, total, sems,
):
    j = pl.program_id(0)
    slot = j % 2
    width = z.shape[1]
    blocks = z.shape[0] // ROW_BLOCK
    weights = (w_g, s_g, w_u, s_u, w_d, s_d)
    ffn_start(weights, offsets, buffers, sems, (0, 1, 2), columns)

    @pl.when(j == 0)
    def _():
        mid = dot(z[...], enter[...], BF16)
        mid_gu[...] = mid
        joined[:, :width] = z[...]
        joined[:, width:] = mid

    def step(count):
        def wait(k):
            for c in ffn_fetch(weights, offsets, buffers, sems, k, j, slot, count):
                c.wait()

        wait(0)
        wait(1)

        @pl.loop(0, blocks)
        def _(i):
            rows = rows_at(i)
            gate_pre = dot(joined[rows, :], buffers[0, slot, :, :count])
            up_pre = dot(joined[rows, :], buffers[1, slot, :, :count])
            value, rate = gelu_parts(gate_pre)
            gelu[rows, :count] = value.astype(BF16)
            slope[rows, :count] = (rate * up_pre).astype(BF16)
            hidden[rows, :count] = (value * up_pre).astype(BF16)

        wait(2)
        add_to(total, dot_nt(hidden[:, :count], buffers[2, slot, :, :count]))

    by_width(columns, step)

    @pl.when(j == pl.num_programs(0) - 1)
    def _():
        mid = total[:, width:].astype(BF16)
        mid_d[...] = mid
        share[...] = (total[:, :width] + dot(mid, leave[...])).astype(BF16)


def ffn_forward(z, enter, leave, weights, offsets):
    length, width = z.shape
    columns = weights[1].shape[1]
    steps = pl.cdiv(columns, FFN_BLOCK)

    def fixed(shape):
        return pl.BlockSpec(shape, lambda j: (0, 0), pipeline_mode=pl.Buffered(1))

    wide = pl.BlockSpec((length, FFN_BLOCK), lambda j: (0, j))
    hbm = pl.BlockSpec(memory_space=pl.ANY)
    small = (length, LANES)
    return pl.pallas_call(
        functools.partial(ffn_forward_kernel, offsets, columns),
        grid=(steps,),
        out_shape=[jax.ShapeDtypeStruct((length, columns), BF16)] * 3
        + [jax.ShapeDtypeStruct(small, BF16)] * 2
        + [jax.ShapeDtypeStruct((length, width), BF16)],
        in_specs=[fixed(z.shape), fixed(enter.shape), fixed(leave.shape)] + [hbm] * 6,
        out_specs=[wide] * 3 + [fixed(small), fixed(small), fixed((length, width))],
        scratch_shapes=[
            pltpu.VMEM((3, 2, width + LANES, FFN_BLOCK), BF16),
            pltpu.VMEM((length, width + LANES), BF16),
            pltpu.VMEM((length, width + LANES), F32),
            pltpu.SemaphoreType.DMA((3, 2, 2)),
        ],
        compiler_params=pltpu.CompilerParams(vmem_limit_bytes=VMEM_LIMIT),
        name="ffn_forward",
    )(z, enter, leave, *weights)


def ffn_gate_kernel(offsets, columns, z, enter, w_g, s_g, gelu, rate, mid_gu, buffers, joined, sems):
    j = pl.program_id(0)
    slot = j % 2
    width = z.shape[1]
    blocks = z.shape[0] // ROW_BLOCK
    ffn_start((w_g, s_g), offsets, buffers, sems, (0,), columns)

    @pl.when(j == 0)
    def _():
        mid = dot(z[...], enter[...], BF16)
        mid_gu[...] = mid
        joined[:, :width] = z[...]
        joined[:, width:] = mid

    def step(count):
        for c in ffn_fetch((w_g, s_g), offsets, buffers, sems, 0, j, slot, count):
            c.wait()

        @pl.loop(0, blocks)
        def _(i):
            rows = rows_at(i)
            value, change = gelu_parts(dot(joined[rows, :], buffers[0, slot, :, :count]))
            gelu[rows, :count] = value.astype(BF16)
            rate[rows, :count] = change.astype(BF16)

    by_width(columns, step)


def ffn_gate(z, enter, weights):
    length, width = z.shape
    columns = weights[1].shape[1]

    def fixed(shape):
        return pl.BlockSpec(shape, lambda j: (0, 0), pipeline_mode=pl.Buffered(1))

    wide = pl.BlockSpec((length, FFN_BLOCK), lambda j: (0, j))
    return pl.pallas_call(
        functools.partial(ffn_gate_kernel, (0,), columns),
        grid=(pl.cdiv(columns, FFN_BLOCK),),
        out_shape=[jax.ShapeDtypeStruct((length, columns), BF16)] * 2
        + [jax.ShapeDtypeStruct((length, LANES), BF16)],
        in_specs=[fixed(z.shape), fixed(enter.shape)] + [pl.BlockSpec(memory_space=pl.ANY)] * 2,
        out_specs=[wide, wide, fixed((length, LANES))],
        scratch_shapes=[
            pltpu.VMEM((1, 2, width + LANES, FFN_BLOCK), BF16),
            pltpu.VMEM((length, width + LANES), BF16),
            pltpu.SemaphoreType.DMA((1, 2, 2)),
        ],
        compiler_params=pltpu.CompilerParams(vmem_limit_bytes=VMEM_LIMIT),
        name="ffn_gate",
    )(z, enter, *weights)


def ffn_rest_kernel(
    offsets, columns, z, mid_gu, leave, gelu, rate, w_u, s_u, w_d, s_d,
    slope, hidden, mid_d, share, buffers, joined, total, sems,
):
    j = pl.program_id(0)
    slot = j % 2
    width = z.shape[1]
    blocks = z.shape[0] // ROW_BLOCK
    weights = (w_u, s_u, w_d, s_d)
    ffn_start(weights, offsets, buffers, sems, (0, 1), columns)

    @pl.when(j == 0)
    def _():
        joined[:, :width] = z[...]
        joined[:, width:] = mid_gu[...]

    def step(count):
        def wait(k):
            for c in ffn_fetch(weights, offsets, buffers, sems, k, j, slot, count):
                c.wait()

        wait(0)

        @pl.loop(0, blocks)
        def _(i):
            rows = rows_at(i)
            up_pre = dot(joined[rows, :], buffers[0, slot, :, :count])
            slope[rows, :count] = (rate[rows, :count].astype(F32) * up_pre).astype(BF16)
            hidden[rows, :count] = (gelu[rows, :count].astype(F32) * up_pre).astype(BF16)

        wait(1)
        add_to(total, dot_nt(hidden[:, :count], buffers[1, slot, :, :count]))

    by_width(columns, step)

    @pl.when(j == pl.num_programs(0) - 1)
    def _():
        mid = total[:, width:].astype(BF16)
        mid_d[...] = mid
        share[...] = (total[:, :width] + dot(mid, leave[...])).astype(BF16)


def ffn_rest(z, mid_gu, leave, gelu, rate, weights, offsets):
    length, width = z.shape
    columns = weights[1].shape[1]

    def fixed(shape):
        return pl.BlockSpec(shape, lambda j: (0, 0), pipeline_mode=pl.Buffered(1))

    wide = pl.BlockSpec((length, FFN_BLOCK), lambda j: (0, j))
    small = (length, LANES)
    return pl.pallas_call(
        functools.partial(ffn_rest_kernel, offsets, columns),
        grid=(pl.cdiv(columns, FFN_BLOCK),),
        out_shape=[jax.ShapeDtypeStruct((length, columns), BF16)] * 2
        + [jax.ShapeDtypeStruct(small, BF16), jax.ShapeDtypeStruct((length, width), BF16)],
        in_specs=[fixed(z.shape), fixed(small), fixed(leave.shape), wide, wide]
        + [pl.BlockSpec(memory_space=pl.ANY)] * 4,
        out_specs=[wide, wide, fixed(small), fixed((length, width))],
        scratch_shapes=[
            pltpu.VMEM((2, 2, width + LANES, FFN_BLOCK), BF16),
            pltpu.VMEM((length, width + LANES), BF16),
            pltpu.VMEM((length, width + LANES), F32),
            pltpu.SemaphoreType.DMA((2, 2, 2)),
        ],
        compiler_params=pltpu.CompilerParams(vmem_limit_bytes=VMEM_LIMIT),
        name="ffn_rest",
    )(z, mid_gu, leave, gelu, rate, *weights)


def ffn_backward_kernel(
    offsets, columns, grad, z, enter, leave, mid_gu, mid_d, spread, gelu, slope, hidden,
    w_g, s_g, w_u, s_u, w_d, s_d,
    share, exit_g, exit_u, entry_d, exit_d, entry_gu,
    buffers, joined, grad_g, grad_u, total, spread_d, spread_gu, sems,
):
    j = pl.program_id(0)
    slot = j % 2
    width = z.shape[1]
    blocks = z.shape[0] // ROW_BLOCK
    weights = (w_g, s_g, w_u, s_u, w_d, s_d)
    ffn_start(weights, offsets, buffers, sems, (2, 0, 1), columns)

    @pl.when(j == 0)
    def _():
        mid = dot_nt(grad[...], leave[...], BF16)
        joined[:, :width] = grad[...]
        joined[:, width:] = mid
        spread_d[...] = dot(mid, spread[:, :LANES], BF16)
        exit_d[...] = (ADAPTER_SCALING * dot_tn(mid_d[...], grad[...]))[:RANK].astype(BF16)

    def step(count):
        def wait(k):
            for c in ffn_fetch(weights, offsets, buffers, sems, k, j, slot, count):
                c.wait()

        wait(2)

        @pl.loop(0, blocks)
        def _(i):
            rows = rows_at(i)
            grad_hidden = dot(joined[rows, :], buffers[2, slot, :, :count])
            grad_g[rows, :count] = (grad_hidden * slope[rows, :count].astype(F32)).astype(BF16)
            grad_u[rows, :count] = (grad_hidden * gelu[rows, :count].astype(F32)).astype(BF16)

        exit_g[:, :count] = (ADAPTER_SCALING * dot_tn(mid_gu[...], grad_g[:, :count]))[:RANK].astype(BF16)
        exit_u[:, :count] = (ADAPTER_SCALING * dot_tn(mid_gu[...], grad_u[:, :count]))[
            RANK : 2 * RANK
        ].astype(BF16)
        wait(0)
        wait(1)
        add_to(
            total,
            dot_nt(grad_g[:, :count], buffers[0, slot, :, :count])
            + dot_nt(grad_u[:, :count], buffers[1, slot, :, :count]),
        )

        @pl.loop(0, count // LANES)
        def _(i):
            wide = dot_tn(hidden[:, rows_at(i, LANES)], spread_d[...])
            entry_d[rows_at(i, RANK), :] = fold_rows(wide)

    by_width(columns, step)

    @pl.when(j == pl.num_programs(0) - 1)
    def _():
        mid = total[:, width:].astype(BF16)
        share[...] = (total[:, :width] + dot_nt(mid, enter[...])).astype(BF16)
        spread_gu[...] = dot(mid, spread[...], BF16)

        @pl.loop(0, width // LANES)
        def _(i):
            wide = dot_tn(z[:, rows_at(i, LANES)], spread_gu[...])
            entry_gu[rows_at(i, RANK), :] = fold_rows(wide)


def ffn_backward(grad, z, enter, leave, kept, weights, offsets):
    length, width = z.shape
    columns = weights[1].shape[1]
    steps = pl.cdiv(columns, FFN_BLOCK)
    spread = jnp.concatenate([slot_spread(i) for i in range(2)], axis=1)

    def fixed(shape):
        return pl.BlockSpec(shape, lambda j: (0, 0), pipeline_mode=pl.Buffered(1))

    wide = pl.BlockSpec((length, FFN_BLOCK), lambda j: (0, j))
    hbm = pl.BlockSpec(memory_space=pl.ANY)
    small = (length, LANES)
    shapes = [
        (length, width), (RANK, columns), (RANK, columns), (columns // GROUPS, LANES), (RANK, width),
        (width // GROUPS, 2 * LANES),
    ]
    narrow = pl.BlockSpec((RANK, FFN_BLOCK), lambda j: (0, j))
    return pl.pallas_call(
        functools.partial(ffn_backward_kernel, offsets, columns),
        grid=(steps,),
        out_shape=[jax.ShapeDtypeStruct(shape, BF16) for shape in shapes],
        in_specs=[
            fixed(grad.shape), fixed(z.shape), fixed(enter.shape), fixed(leave.shape), fixed(small),
            fixed(small), fixed(spread.shape), wide, wide, wide,
        ] + [hbm] * 6,
        out_specs=[
            fixed((length, width)), narrow, narrow,
            pl.BlockSpec((FFN_BLOCK // GROUPS, LANES), lambda j: (j, 0)),
            fixed((RANK, width)), fixed((width // GROUPS, 2 * LANES)),
        ],
        scratch_shapes=[
            pltpu.VMEM((3, 2, width + LANES, FFN_BLOCK), BF16),
            pltpu.VMEM((length, width + LANES), BF16),
            pltpu.VMEM((length, FFN_BLOCK), BF16),
            pltpu.VMEM((length, FFN_BLOCK), BF16),
            pltpu.VMEM((length, width + LANES), F32),
            pltpu.VMEM(small, BF16),
            pltpu.VMEM((length, 2 * LANES), BF16),
            pltpu.SemaphoreType.DMA((3, 2, 2)),
        ],
        compiler_params=pltpu.CompilerParams(vmem_limit_bytes=VMEM_LIMIT),
        name="ffn_backward",
    )(
        grad, z, enter, leave, kept["mid_gu"], kept["mid_d"], spread, kept["gelu"], kept["slope"],
        kept["hidden"], *weights,
    )


def piece_starts(layer_idx):
    starts, at = {}, layer_idx * sum(n for _, n in PIECES) * RANK // LANES
    for name, n in PIECES:
        starts[name] = at
        at += n * RANK // LANES
    return starts


def unpack_kernel(head_cols, hidden_cols, rows, *refs):
    outs, (values, tall) = refs[:-2], refs[-2:]
    tp_place = lax.axis_index("tp")
    sizes = dict(PIECES)

    @pl.loop(0, rows.shape[0] // 16)
    def _(i):
        at = pl.ds(pl.multiple_of(i * 16, 16), 16)
        values[at, :] = rows[at, :].astype(F32)

    def entries(names, starts, count):
        lane = lax.broadcasted_iota(jnp.int32, (count, LANES), 1)
        for s in range(GROUPS):
            row = jnp.zeros((count, LANES), F32)
            for i, start in enumerate(starts):
                moved = values[pl.ds(start, count), :]
                if (i - s) % GROUPS:
                    moved = pltpu.roll(moved, (i - s) % GROUPS * RANK, 1)
                row = jnp.where(lane // RANK == i, moved, row)
            tall[pl.ds(s, count, stride=GROUPS), :] = row

    def exit_rows(out, start, stride, columns, slot, scale):
        for j in range((columns.stop - columns.start) // LANES):
            block = values[pl.ds(start + j, RANK, stride=stride), :] * scale
            at = columns.start + j * LANES
            out[slot * RANK : (slot + 1) * RANK, at : at + LANES] = block.astype(BF16)

    for l in range(LAYERS):
        starts = piece_starts(l)
        enter_qkv, enter_gu, leave_o, leave_d, s_qkv, s_o, s_g, s_u, s_d = outs[9 * l : 9 * l + 9]
        for out in (leave_o, leave_d, s_qkv, s_g, s_u):
            out[...] = jnp.zeros_like(out)
        for out, names in ((enter_qkv, ("Eq", "Ek", "Ev")), (enter_gu, ("Eg", "Eu"))):
            entries(names, [starts[n] for n in names], D // GROUPS)
            out[...] = tall[:D, :].astype(BF16)
        for out, name, columns in ((s_o, "Eo", head_cols), (s_d, "Ed", hidden_cols)):
            count = columns // GROUPS
            entries((name,), [pl.multiple_of(starts[name] + tp_place * count, 8)], count)
            for j in range(columns // LANES):
                at = slice(j * LANES, (j + 1) * LANES)
                out[:, at] = tall[at, :].T.astype(BF16)
        exit_rows(leave_o, starts["Xo"], D // LANES, slice(0, D), 0, ADAPTER_SCALING)
        exit_rows(leave_d, starts["Xd"], D // LANES, slice(0, D), 0, ADAPTER_SCALING)
        for out, name, columns, slot in (
            (s_qkv, "Xq", slice(0, head_cols), 0),
            (s_qkv, "Xk", slice(head_cols, head_cols + HD), 1),
            (s_qkv, "Xv", slice(head_cols + HD, head_cols + 2 * HD), 2),
            (s_g, "Xg", slice(0, hidden_cols), 0),
            (s_u, "Xu", slice(0, hidden_cols), 1),
        ):
            stride = sizes[name] // LANES
            width = (columns.stop - columns.start) // LANES
            first = starts[name] + (tp_place * width if width < stride else 0)
            exit_rows(out, first, stride, columns, slot, ADAPTER_SCALING)


def unpack(own_rows, head_cols, hidden_cols):
    shapes = [
        (D, LANES), (D, LANES), (LANES, D), (LANES, D), (LANES, head_cols + 2 * HD),
        (LANES, head_cols), (LANES, hidden_cols), (LANES, hidden_cols), (LANES, hidden_cols),
    ]
    vmem = pl.BlockSpec(memory_space=pltpu.VMEM)
    got = pl.pallas_call(
        functools.partial(unpack_kernel, head_cols, hidden_cols),
        out_shape=[jax.ShapeDtypeStruct(shape, BF16) for shape in shapes * LAYERS],
        in_specs=[vmem],
        out_specs=[vmem] * (len(shapes) * LAYERS),
        scratch_shapes=[
            pltpu.VMEM(own_rows.shape, F32), pltpu.VMEM((max(D, hidden_cols), LANES), F32),
        ],
        name="unpack",
    )(own_rows)
    maps, spares = [], []
    for l in range(LAYERS):
        part = got[9 * l : 9 * l + 9]
        maps.append(dict(zip(("enter_qkv", "enter_gu", "leave_o", "leave_d"), part)))
        spares.append(dict(zip(("qkv", "o", "g", "u", "d"), part[4:])))
    return maps, spares


def shards(
    hidden_in, out_grad, segments, positions, set_ids, query_w, key_w, value_w, out_w, gate_w,
    up_w, down_w, norm_gains, head_gains, adapters, first_moment, second_moment,
):
    tp_count = lax.axis_size("tp")
    fsdp_count = lax.axis_size("fsdp")
    tp_place = lax.axis_index("tp")
    set_count, share = adapters.shape
    head_cols = HEADS * HD // tp_count
    hidden_cols = FF // tp_count
    scale = HD ** (-0.5)
    set_range = jnp.arange(set_count, dtype=jnp.int32)

    selector = (set_ids[:, None] == set_range[None, :]).astype(BF16)
    whole_rows = share % LANES == 0
    tile = (share // LANES, LANES) if whole_rows else (1, share)

    def core_half(w):
        return lax.dynamic_slice_in_dim(w, tp_place * (HD // tp_count), HD // tp_count, 1)

    def local_weights(l):
        return {
            "qkv": jnp.concatenate([query_w[l], core_half(key_w[l]), core_half(value_w[l])], axis=1),
            "o": out_w[l].T,
            "g": gate_w[l],
            "u": up_w[l],
            "d": down_w[l].T,
        }

    local = [local_weights(l) for l in range(LAYERS)]
    first_names = [(0, "qkv"), (0, "o"), (0, "g"), (0, "u"), (0, "d"), (1, "qkv"), (1, "o"), (1, "g")]
    late = jnp.concatenate([local[1]["u"], local[1]["d"]], axis=1)
    arrays = [local[l][name] for l, name in first_names]
    if fsdp_count == 16:
        part = hidden_cols * 4 // 9 // LANES * LANES
        plan = [
            ("zxy", 0, (0, arrays[0].shape[1])), ("zxy", 1, (0, arrays[1].shape[1])),
            ("zyx", 5, (0, arrays[5].shape[1])), ("zyx", 6, (0, arrays[6].shape[1])),
            ("zxy", 2, (0, hidden_cols)), ("zyx", 3, (0, hidden_cols)),
            ("xyz", 4, (part, hidden_cols - part)), ("yxz", 7, (part, hidden_cols - part)),
            ("zxy", 4, (0, part)), ("zyx", 7, (0, part)),
        ]
        first = gather_weights(arrays, plan, fsdp_count, 11)
    else:
        first = [lax.all_gather(a, "fsdp", axis=0, tiled=True) for a in arrays]
    master_low, late, first = lax.optimization_barrier((adapters, late, first))
    late_all = lax.all_gather(late, "fsdp", axis=0, tiled=True)
    routed = dot(selector, master_low.astype(BF16), BF16).reshape((fsdp_count,) + tile)
    own = lax.all_to_all(routed, "fsdp", split_axis=0, concat_axis=0, tiled=True)

    own, key_values = pair_gather(own, [first[first_names.index((l, "qkv"))] for l in range(LAYERS)], HD, 13)
    own_rows = own.reshape(-1, LANES) if whole_rows else own.reshape(-1).reshape(-1, LANES)
    maps, spares = unpack(own_rows, head_cols, hidden_cols)

    weights = [dict(), dict()]
    for (l, name), array in zip(first_names, first):
        weights[l][name] = (array, spares[l][name]) + ((key_values[l],) if name == "qkv" else ())
    weights[1]["u"] = (late_all, spares[1]["u"])
    weights[1]["d"] = (late_all, spares[1]["d"])
    ffn_weights = [w["g"] + w["u"] + w["d"] for w in weights]
    ffn_offsets = [(0, 0, 0), (0, 0, hidden_cols)]
    cosine, sine = rope_tables(positions)
    gains = norm_gains.astype(F32)
    heads = head_gains.astype(F32)

    def gain(l, i):
        return gains[l, i][None, :]

    kept = []
    normed = exchange(body_enter, 1, "enter", None, [hidden_in], [gain(0, 0)], [], True)[0]
    x = hidden_in
    for l in range(LAYERS):
        w = weights[l]
        r = {"x": x, "normed": normed}
        m = maps[l]
        (
            r["raw"], r["qkv"], r["attn"], r["mid_qkv"], r["mid_o"], r["stats"], share_o,
        ) = attention_forward(
            normed, m["enter_qkv"], m["leave_o"], heads[l], cosine, sine, segments, w["qkv"],
            w["o"], scale,
        )
        r["attn_branch"], r["middle"], r["normed_two"] = exchange(
            body_middle, 2 if l == 0 else 3, "middle", share_o, [x], [gain(l, 1), gain(l, 2)],
            [F32, F32], True,
        )
        if l == 0:
            r["gelu"], r["slope"], r["hidden"], r["mid_gu"], r["mid_d"], share_f = ffn_forward(
                r["normed_two"], m["enter_gu"], m["leave_d"], ffn_weights[l], ffn_offsets[l]
            )
        else:
            r["gelu"], rate, r["mid_gu"] = ffn_gate(r["normed_two"], m["enter_gu"], w["g"])
            r["slope"], r["hidden"], r["mid_d"], share_f = ffn_rest(
                r["normed_two"], r["mid_gu"], m["leave_d"], r["gelu"], rate, w["u"] + w["d"],
                ffn_offsets[l][1:],
            )
        if l + 1 < LAYERS:
            r["ffn_branch"], x, normed = exchange(
                body_next, 4, "next", share_f, [r["middle"]], [gain(l, 3), gain(l + 1, 0)],
                [F32, F32], True,
            )
        else:
            result, grad_ffn = exchange(
                body_turn, 5, "turn", share_f, [r["middle"], out_grad], [gain(l, 3)], [BF16], True
            )
        kept.append(r)

    grad_out = out_grad
    layer_grads = [None] * LAYERS
    for l in reversed(range(LAYERS)):
        w, r, m = weights[l], kept[l], maps[l]
        pieces = {}

        share_n2, pieces["Xg"], pieces["Xu"], pieces["Ed"], pieces["Xd"], entry_gu = ffn_backward(
            grad_ffn, r["normed_two"], m["enter_gu"], m["leave_d"], r, ffn_weights[l], ffn_offsets[l]
        )
        pieces["Eg"], pieces["Eu"] = entry_gu[:, :LANES], entry_gu[:, LANES:]
        grad_middle, grad_branch = exchange(
            body_back_middle, 6 if l == 1 else 7, "back_middle", share_n2,
            [grad_out, r["middle"], r["attn_branch"]], [gain(l, 2), gain(l, 1)], [F32], True,
        )
        share_n, entry_qkv, pieces["Eo"], exit_qkv, pieces["Xo"] = attention_backward(
            grad_branch, m["enter_qkv"], m["leave_o"], heads[l], cosine, sine, segments, r, w["qkv"],
            w["o"], scale,
        )
        for i, name in enumerate("qkv"):
            pieces["E" + name] = entry_qkv[:, i * LANES : (i + 1) * LANES]
        pieces["Xq"] = exit_qkv[:, :head_cols]
        pieces["Xk"] = exit_qkv[:, head_cols : head_cols + HD]
        pieces["Xv"] = exit_qkv[:, head_cols + HD :]
        if l > 0:
            grad_out, grad_ffn = exchange(
                body_back_next, 8, "back_next", share_n,
                [grad_middle, r["x"], kept[l - 1]["ffn_branch"]], [gain(l, 0), gain(l - 1, 3)],
                [F32], True,
            )
        else:
            grad_out = exchange(
                body_back_last, 9, "back_last", share_n, [grad_middle, r["x"]], [gain(l, 0)], [F32], False
            )[0]
        rows = []
        for name, n in PIECES:
            piece = pieces[name]
            if name in ("Eo", "Ed"):
                piece = lax.dynamic_update_slice_in_dim(
                    jnp.zeros((n * RANK // LANES, LANES), BF16), piece, tp_place * piece.shape[0], 0
                )
            if name in ("Xq", "Xg", "Xu"):
                piece = lax.dynamic_update_slice_in_dim(
                    jnp.zeros((RANK, n), BF16), piece, tp_place * piece.shape[1], 1
                )
            rows.append(piece.reshape(-1, LANES))
        layer_grads[l] = rows

    flat = jnp.concatenate(layer_grads[0] + layer_grads[1], axis=0)
    if whole_rows:
        flat = flat.reshape(fsdp_count * tp_count, share // LANES, LANES)
    else:
        flat = flat.reshape(-1).reshape(fsdp_count * tp_count, 1, share)
    chip_sum = pair_sum(flat, 10)
    arrived = lax.all_to_all(chip_sum, "fsdp", split_axis=0, concat_axis=0, tiled=True).reshape(fsdp_count, share)
    owner_pick = (set_range[:, None] == set_ids[None, :]).astype(BF16)
    set_grads = dot(owner_pick, arrived)
    first_new = BETA_ONE * first_moment + (1.0 - BETA_ONE) * set_grads
    second_new = BETA_TWO * second_moment + (1.0 - BETA_TWO) * set_grads * set_grads
    first_hat = first_new / (1.0 - BETA_ONE**ADAM_STEPS)
    second_hat = second_new / (1.0 - BETA_TWO**ADAM_STEPS)
    new_master = adapters - LEARN_RATE * (
        first_hat / (jnp.sqrt(second_hat) + ADAM_EPS) + DECAY_RATE * adapters
    )
    return (
        result, grad_out, set_grads, new_master, first_new, second_new, new_master.astype(BF16),
    )


def solution(mesh):
    return jax.shard_map(
        shards,
        mesh=mesh,
        in_specs=(
            P(("fsdp", "tp"), None),
            P(("fsdp", "tp"), None),
            P("fsdp"),
            P("fsdp"),
            P(),
            P(None, "fsdp", "tp"),
            P(None, "fsdp", None),
            P(None, "fsdp", None),
            P(None, "tp", "fsdp"),
            P(None, "fsdp", "tp"),
            P(None, "fsdp", "tp"),
            P(None, "tp", "fsdp"),
            P(),
            P(),
            P(None, ("fsdp", "tp")),
            P(None, ("fsdp", "tp")),
            P(None, ("fsdp", "tp")),
        ),
        out_specs=(
            P(("fsdp", "tp"), None),
            P(("fsdp", "tp"), None),
            P(None, ("fsdp", "tp")),
            P(None, ("fsdp", "tp")),
            P(None, ("fsdp", "tp")),
            P(None, ("fsdp", "tp")),
            P(None, ("fsdp", "tp")),
        ),
        check_vma=False,
    )
```
